128 devices in a mesh: dp: 1, tp: 2 (over core), sp: 64 (over z, y, x).
Axes of the slice: x: 4, y: 4, z: 4, core: 2. Of those that a mesh axis runs over, the one named last changes fastest.
Arguments:
- tok_emb: bfloat16 [4, 32, 1536], P(None, 'dp')
- lengths: int32 [32], P('dp')
- key_cache: bfloat16 [2, 32, 8192, 2, 128], P(None, 'dp', 'sp', 'tp')
- val_cache: bfloat16 [2, 32, 8192, 2, 128], P(None, 'dp', 'sp', 'tp')
- gain_attn: bfloat16 [2, 1536], replicated
- gain_mlp: bfloat16 [2, 1536], replicated
- w_query: bfloat16 [2, 1536, 1536], P(None, None, 'tp')
- w_key: bfloat16 [2, 1536, 256], P(None, None, 'tp')
- w_value: bfloat16 [2, 1536, 256], P(None, None, 'tp')
- w_out: bfloat16 [2, 1536, 1536], P(None, 'tp')
- w_gate: bfloat16 [2, 1536, 8960], P(None, None, 'tp')
- w_up: bfloat16 [2, 1536, 8960], P(None, None, 'tp')
- w_down: bfloat16 [2, 8960, 1536], P(None, 'tp')
Outputs:
- output 1: bfloat16 [4, 32, 1536], P(None, 'dp')
- output 2: bfloat16 [2, 32, 8192, 2, 128], P(None, 'dp', 'sp', 'tp')
- output 3: bfloat16 [2, 32, 8192, 2, 128], P(None, 'dp', 'sp', 'tp')
All inputs are finite; a program needn't handle non-finite values.
Results may differ from the reference program's by a relative error of at most 0.0151098.
Values sent between devices are 32-bit elements.
A program may use at most 1 GiB of HBM per device.

```python
import math
import jax
import jax.numpy as jnp
from jax import lax

N_STEPS = 4
N_LAYERS = 2
SEQ_BATCH = 32
LOC_LEN = 128
SP_SIZE = 64
D_MODEL = 1536
N_HEADS = 12
KV_HEADS = 2
HEAD_DIM = 128
FF_DIM = 8960
CACHE_LEN = LOC_LEN * SP_SIZE
GROUP_SIZE = N_HEADS // KV_HEADS
EPS = 1e-5
ROPE_BASE = 500000.0


def draw_lengths(len_key, perm_key):
    drawn_len = jax.random.randint(len_key, (SEQ_BATCH,), CACHE_LEN // 2, CACHE_LEN - N_STEPS + 1)
    perm_ids = jax.random.permutation(perm_key, SEQ_BATCH)
    lengths = jnp.where(perm_ids == 0, CACHE_LEN - N_STEPS, jnp.where(perm_ids == 1, CACHE_LEN // 2, drawn_len))
    return lengths.astype(jnp.int32)


def draw_scales():
    score_var = max(math.log(CACHE_LEN / 32.0), 1.0)
    plant_gain = (math.log(CACHE_LEN) + 0.5 * score_var) / math.sqrt(HEAD_DIM)
    key_scale = math.sqrt(score_var / (1.0 + plant_gain * plant_gain))
    return plant_gain, key_scale


def setup_inputs(seed: int = 0, part: int = 0) -> dict:
    plant_gain, key_scale = draw_scales()
    part_keys = jax.random.split(jax.random.fold_in(jax.random.key(seed), part), 6)
    weight_keys = jax.random.split(jax.random.key(seed + 1), 9)
    common = jax.random.normal(part_keys[0], (SEQ_BATCH, D_MODEL), jnp.float32)
    step_noise = jax.random.normal(part_keys[1], (N_STEPS, SEQ_BATCH, D_MODEL), jnp.float32)
    tok_emb = ((common[None] + 0.4 * step_noise) / math.sqrt(1.16)).astype(jnp.bfloat16)
    lengths = draw_lengths(part_keys[2], part_keys[3])
    cache_shape = (N_LAYERS, SEQ_BATCH, CACHE_LEN, KV_HEADS, HEAD_DIM)
    key_cache = (key_scale * jax.random.normal(part_keys[4], cache_shape, jnp.float32)).astype(jnp.bfloat16)
    val_cache = jax.random.normal(part_keys[5], cache_shape, jnp.float32).astype(jnp.bfloat16)
    gain_attn = (1.0 + 0.3 * jax.random.normal(weight_keys[0], (N_LAYERS, D_MODEL), jnp.float32)).astype(jnp.bfloat16)
    gain_mlp = (1.0 + 0.3 * jax.random.normal(weight_keys[1], (N_LAYERS, D_MODEL), jnp.float32)).astype(jnp.bfloat16)
    in_scale = D_MODEL ** -0.5
    key_proj = jax.random.normal(weight_keys[2], (N_LAYERS, D_MODEL, KV_HEADS, HEAD_DIM), jnp.float32) * in_scale
    query_proj = plant_gain * jnp.repeat(key_proj, GROUP_SIZE, axis=2) + jax.random.normal(weight_keys[3], (N_LAYERS, D_MODEL, N_HEADS, HEAD_DIM), jnp.float32) * in_scale
    w_query = query_proj.reshape(N_LAYERS, D_MODEL, N_HEADS * HEAD_DIM).astype(jnp.bfloat16)
    w_key = key_proj.reshape(N_LAYERS, D_MODEL, KV_HEADS * HEAD_DIM).astype(jnp.bfloat16)
    w_value = (jax.random.normal(weight_keys[4], (N_LAYERS, D_MODEL, KV_HEADS * HEAD_DIM), jnp.float32) * in_scale).astype(jnp.bfloat16)
    w_out = (jax.random.normal(weight_keys[5], (N_LAYERS, N_HEADS * HEAD_DIM, D_MODEL), jnp.float32) * (N_HEADS * HEAD_DIM) ** -0.5).astype(jnp.bfloat16)
    w_gate = (jax.random.normal(weight_keys[6], (N_LAYERS, D_MODEL, FF_DIM), jnp.float32) * in_scale).astype(jnp.bfloat16)
    w_up = (jax.random.normal(weight_keys[7], (N_LAYERS, D_MODEL, FF_DIM), jnp.float32) * in_scale).astype(jnp.bfloat16)
    w_down = (jax.random.normal(weight_keys[8], (N_LAYERS, FF_DIM, D_MODEL), jnp.float32) * FF_DIM ** -0.5).astype(jnp.bfloat16)
    return {'tok_emb': tok_emb, 'lengths': lengths, 'key_cache': key_cache, 'val_cache': val_cache, 'gain_attn': gain_attn, 'gain_mlp': gain_mlp, 'w_query': w_query, 'w_key': w_key, 'w_value': w_value, 'w_out': w_out, 'w_gate': w_gate, 'w_up': w_up, 'w_down': w_down}


def rms_norm(hidden, gain_vec):
    x_float = hidden.astype(jnp.float32)
    inv_rms = lax.rsqrt(jnp.mean(x_float * x_float, axis=-1, keepdims=True) + EPS)
    return (x_float * inv_rms * gain_vec.astype(jnp.float32)).astype(jnp.bfloat16)


def rotary(in_vecs, positions):
    head_dim = in_vecs.shape[-1]
    half_dim = head_dim // 2
    inv_freq = 1.0 / (ROPE_BASE ** (jnp.arange(half_dim).astype(jnp.float32) * 2.0 / head_dim))
    angles = positions.astype(jnp.float32)[:, None] * inv_freq[None, :]
    cos_a = jnp.cos(angles)[:, None, :]
    sin_a = jnp.sin(angles)[:, None, :]
    front_half = in_vecs[..., :half_dim]
    back_half = in_vecs[..., half_dim:]
    return jnp.concatenate([front_half * cos_a - back_half * sin_a, back_half * cos_a + front_half * sin_a], axis=-1)


def reference(tok_emb, lengths, key_cache, val_cache, gain_attn, gain_mlp, w_query, w_key, w_value, w_out, w_gate, w_up, w_down):
    slot_ids = jnp.arange(CACHE_LEN)
    slot_pos = (slot_ids % LOC_LEN) * SP_SIZE + slot_ids // LOC_LEN
    row_ids = jnp.arange(SEQ_BATCH)

    def one_step(caches, step_in):
        step_idx, hidden = step_in
        cur_pos = lengths + step_idx
        write_slot = (cur_pos % SP_SIZE) * LOC_LEN + cur_pos // SP_SIZE
        valid_mask = (slot_pos[None, :] <= cur_pos[:, None])[:, None, None, :]

        def one_layer(hidden, layer_in):
            lay_k, lay_v, gain_a, gain_m, lay_wq, lay_wk, lay_wv, lay_wo, lay_wg, lay_wu, lay_wd = layer_in
            normed = rms_norm(hidden, gain_a)
            q_vec = jnp.dot(normed, lay_wq, preferred_element_type=jnp.float32).reshape(SEQ_BATCH, N_HEADS, HEAD_DIM)
            k_vec = jnp.dot(normed, lay_wk, preferred_element_type=jnp.float32).reshape(SEQ_BATCH, KV_HEADS, HEAD_DIM)
            v_vec = jnp.dot(normed, lay_wv, preferred_element_type=jnp.float32).reshape(SEQ_BATCH, KV_HEADS, HEAD_DIM).astype(jnp.bfloat16)
            q_rot = rotary(q_vec, cur_pos).astype(jnp.bfloat16).reshape(SEQ_BATCH, KV_HEADS, GROUP_SIZE, HEAD_DIM)
            k_rot = rotary(k_vec, cur_pos).astype(jnp.bfloat16)
            lay_k = lay_k.at[row_ids, write_slot].set(k_rot)
            lay_v = lay_v.at[row_ids, write_slot].set(v_vec)
            scores = jnp.einsum('bkgd,bjkd->bkgj', q_rot.astype(jnp.float32), lay_k.astype(jnp.float32)) * HEAD_DIM ** -0.5
            scores = jnp.where(valid_mask, scores, -1e30)
            prob_w = jnp.exp(scores - jnp.max(scores, axis=-1, keepdims=True))
            denom_sum = jnp.sum(prob_w, axis=-1, keepdims=True)
            numer_sum = jnp.einsum('bkgj,bjkd->bkgd', prob_w.astype(jnp.bfloat16).astype(jnp.float32), lay_v.astype(jnp.float32))
            attn_out = (numer_sum / denom_sum).astype(jnp.bfloat16).reshape(SEQ_BATCH, N_HEADS * HEAD_DIM)
            hidden = (hidden.astype(jnp.float32) + jnp.dot(attn_out, lay_wo, preferred_element_type=jnp.float32)).astype(jnp.bfloat16)
            normed = rms_norm(hidden, gain_m)
            gate_pre = jnp.dot(normed, lay_wg, preferred_element_type=jnp.float32)
            up_pre = jnp.dot(normed, lay_wu, preferred_element_type=jnp.float32)
            mlp_act = (jax.nn.silu(gate_pre) * up_pre).astype(jnp.bfloat16)
            hidden = (hidden.astype(jnp.float32) + jnp.dot(mlp_act, lay_wd, preferred_element_type=jnp.float32)).astype(jnp.bfloat16)
            return hidden, (lay_k, lay_v)

        hidden, new_caches = lax.scan(one_layer, hidden, (caches[0], caches[1], gain_attn, gain_mlp, w_query, w_key, w_value, w_out, w_gate, w_up, w_down))
        return new_caches, hidden

    final_caches, hidden_all = lax.scan(one_step, (key_cache, val_cache), (jnp.arange(N_STEPS), tok_emb))
    return (hidden_all, final_caches[0], final_caches[1])
```

```python
import functools
import jax
import jax.numpy as jnp
from jax import lax
from jax.experimental import pallas as pl
from jax.experimental.pallas import tpu as pltpu
from jax.sharding import PartitionSpec as P

EPS = 1e-5
ROPE_BASE = 500000.0
F32 = jnp.float32
BF16 = jnp.bfloat16
MESH = pl.DeviceIdType.MESH
LANES = 128
MLP_CHUNK = 1280
SEQ_UNROLL = 4


def rms_norm(x, gain):
    inv_rms = lax.rsqrt(jnp.mean(x * x, axis=-1, keepdims=True) + EPS)
    return (x * inv_rms * gain.astype(F32)).astype(BF16)


def dot(a, b):
    return jnp.dot(a, b, preferred_element_type=F32)


def decode_kernel(cfg, emb, kc, vc, wq, wk, wv, wo, wg, wu, wd, cos_ref, sin_ref, lim_ref, wsl_ref, slot_ref, ga, gm,
                  out, ksel_out, vsel_out,
                  emb_v, k_v, v_v, wqkv_v, wo_v, wg_v, wu_v, wd_v, u3, qtmp, qs, limr, ktok, vtok, ksel, vsel,
                  send, recv, pad_a, res, g_v, acc, xs, xr, ag, ubuf,
                  in_sem, kv_sem, qkv_sem, wo_sem, g_sem, u_sem, d_sem,
                  rs_ss, rs_rs, x_ss, x_rs, ag_ss, ag_rs, dd_ss, dd_rs):
    dims, n_steps, n_layers, n_seq, heads, d_model, ff = cfg
    nz, ny, nx = dims
    n_sp = nz * ny * nx
    n_tok = n_steps * n_seq
    blocks = d_model // LANES
    q_cols = heads * LANES
    chunk = min(MLP_CHUNK, ff)
    n_full, tail = ff // chunk, ff % chunk
    me = lax.axis_index('sp')
    core = lax.axis_index('tp')
    other = 1 - core
    start_row = lax.rem(me // (ny * nx) + nz // 2, nz) * ny + lax.rem(lax.rem(me // nx, ny) + ny // 2, ny)
    start_seq = start_row * (nx // 2)

    def at_sp(dst):
        return {'sp': dst}

    barrier = pltpu.get_barrier_semaphore()

    def hello(i, carry):
        peer = lax.rem(me + i, n_sp)
        pl.semaphore_signal(barrier, inc=1, device_id=at_sp(peer), device_id_type=MESH)
        return carry

    lax.fori_loop(1, n_sp, hello, 0)
    pl.semaphore_signal(barrier, inc=1, device_id={'tp': other}, device_id_type=MESH)

    def qkv_copies(layer):
        return [
            pltpu.make_async_copy(wq.at[layer], wqkv_v.at[:, pl.ds(0, q_cols)], qkv_sem.at[0]),
            pltpu.make_async_copy(wk.at[layer], wqkv_v.at[:, pl.ds(q_cols, LANES)], qkv_sem.at[1]),
            pltpu.make_async_copy(wv.at[layer], wqkv_v.at[:, pl.ds(q_cols + LANES, LANES)], qkv_sem.at[2]),
        ]

    def kv_copies(layer):
        return [
            pltpu.make_async_copy(kc.at[layer], k_v.at[layer], kv_sem.at[layer, 0]),
            pltpu.make_async_copy(vc.at[layer], v_v.at[layer], kv_sem.at[layer, 1]),
        ]

    def wo_copy(layer):
        return pltpu.make_async_copy(wo.at[layer], wo_v, wo_sem)

    def cols_copy(hbm, vmem, sem, layer, c, size):
        cols = pl.ds(pl.multiple_of(c * chunk, LANES), size)
        return pltpu.make_async_copy(hbm.at[layer, :, cols], vmem.at[:, cols], sem.at[c])

    def rows_copy(layer, c, size):
        rows = pl.ds(pl.multiple_of(c * chunk, LANES), size)
        return pltpu.make_async_copy(wd.at[layer, rows, :], wd_v.at[rows, :], d_sem.at[c])

    pieces = [(c, chunk) for c in range(n_full)] + ([(n_full, tail)] if tail else [])

    emb_copy = pltpu.make_async_copy(emb, emb_v, in_sem)
    emb_copy.start()
    for copy in qkv_copies(0) + kv_copies(0):
        copy.start()
    wo_copy(0).start()
    for c, size in pieces:
        cols_copy(wg, wg_v, g_sem, 0, c, size).start()
        cols_copy(wu, wu_v, u_sem, 0, c, size).start()
    for c, size in pieces:
        rows_copy(0, c, size).start()
    for copy in kv_copies(1):
        copy.start()

    for r in range(8):
        limr[pl.ds(r, n_tok, stride=8), :] = lim_ref[...]
    zeros = jnp.zeros((n_tok, LANES), F32)
    for r in range(heads, 8):
        qs[pl.ds(r, n_tok, stride=8), :] = zeros
    pad_a[...] = jnp.zeros_like(pad_a)
    res[...] = jnp.zeros_like(res)

    emb_copy.wait()
    for s in range(n_steps):
        for j in range(blocks):
            u3[j, pl.ds(s, n_seq, stride=n_steps), :] = emb_v[s, :, j * LANES:(j + 1) * LANES].astype(F32)
    for t in range(2):
        for j in range(blocks):
            res[t:t + 1, j * LANES:(j + 1) * LANES] = u3[j, pl.ds(2 * me + t, 1), :]

    def exchange(layer, phase, part):
        xs[layer, phase] = part
        copy = pltpu.make_async_remote_copy(
            src_ref=xs.at[layer, phase], dst_ref=xr.at[layer, phase], send_sem=x_ss.at[layer, phase], recv_sem=x_rs.at[layer, phase],
            device_id={'tp': other}, device_id_type=MESH)
        copy.start()
        copy.wait()
        return part + xr[layer, phase]

    for layer in range(n_layers):
        x = jnp.concatenate([u3[j] for j in range(blocks)], axis=-1)
        normed = rms_norm(x, ga[layer:layer + 1, :])
        for copy in qkv_copies(layer):
            copy.wait()
        qkv = dot(normed, wqkv_v[...])
        if layer + 1 < n_layers:
            for copy in qkv_copies(layer + 1):
                copy.start()
        cos_a, sin_a = cos_ref[...], sin_ref[...]

        def rotate(vec):
            return (vec * cos_a + pltpu.roll(vec, LANES // 2, 1) * sin_a).astype(BF16).astype(F32)

        for h in range(heads):
            qs[pl.ds(h, n_tok, stride=8), :] = rotate(qkv[:, h * LANES:(h + 1) * LANES])
        ktok[...] = rotate(qkv[:, q_cols:q_cols + LANES])
        vtok[...] = qkv[:, q_cols + LANES:q_cols + 2 * LANES].astype(BF16).astype(F32)
        k_mine = jnp.zeros((n_seq, LANES), F32)
        v_mine = jnp.zeros((n_seq, LANES), F32)
        for s in range(n_steps):
            mine = wsl_ref[s] >= 0
            k_mine = jnp.where(mine, ktok[pl.ds(s, n_seq, stride=n_steps), :], k_mine)
            v_mine = jnp.where(mine, vtok[pl.ds(s, n_seq, stride=n_steps), :], v_mine)
        ksel[...] = k_mine
        vsel[...] = v_mine
        ksel_out[layer] = k_mine
        vsel_out[layer] = v_mine
        if layer == 0:
            pl.semaphore_wait(barrier, n_sp)
        for copy in kv_copies(layer):
            copy.wait()

        def attend(b):
            slot = slot_ref[pl.ds(b, 1), :]
            here = lax.broadcasted_iota(jnp.int32, (LANES, LANES), 0) == slot
            keys = jnp.where(here, ksel[pl.ds(b, 1), :], k_v[layer, b].astype(F32)).astype(BF16)
            vals = jnp.where(here, vsel[pl.ds(b, 1), :], v_v[layer, b].astype(F32)).astype(BF16)
            rows = pl.ds(pl.multiple_of(b * 8 * n_steps, 8), 8 * n_steps)
            q = qs[rows, :].astype(BF16)
            scores = lax.dot_general(q, keys, (((1,), (1,)), ((), ())), preferred_element_type=F32) * LANES ** -0.5
            valid = lax.broadcasted_iota(jnp.int32, scores.shape, 1) <= limr[rows, :]
            scores = jnp.where(valid, scores, -1e30)
            top = jnp.max(scores, axis=-1, keepdims=True)
            w = jnp.exp(scores - top)
            total = jnp.sum(w, axis=-1, keepdims=True)
            o = dot(w.astype(BF16), vals)
            sub = lax.broadcasted_iota(jnp.int32, (8, LANES), 0)
            lane = lax.broadcasted_iota(jnp.int32, (8, LANES), 1)
            tiles = []
            for t in range(n_steps):
                part = slice(8 * t, 8 * t + 8)
                stat = jnp.where(lane == sub, top[part], jnp.where(lane == sub + LANES // 2, total[part], 0.0))
                stat = jnp.sum(stat, axis=0, keepdims=True)
                tiles.append(jnp.where(sub == heads, stat, o[part]))
            return tiles

        def seq_group(i, carry):
            group = []
            for k in range(SEQ_UNROLL):
                b = lax.rem(start_seq + i * SEQ_UNROLL + k, n_seq)
                group.append((b, attend(b)))
            for b, tiles in group:
                rows = pl.ds(pl.multiple_of(b * 8 * n_steps, 8), 8 * n_steps)
                send[layer, rows, :] = jnp.concatenate(tiles, axis=0)
            for b, tiles in group:
                for half in range(2):
                    dst = 2 * b + half
                    rows = pl.ds(pl.multiple_of(dst * 16, 16), 16)
                    home = pl.ds(pl.multiple_of(me * 16, 16), 16)

                    @pl.when(dst != me)
                    def _():
                        pltpu.make_async_remote_copy(
                            src_ref=send.at[layer, rows, :], dst_ref=recv.at[layer, home, :],
                            send_sem=rs_ss.at[layer], recv_sem=rs_rs.at[layer],
                            device_id=at_sp(dst), device_id_type=MESH).start()

                    @pl.when(dst == me)
                    def _():
                        recv[layer, home, :] = jnp.concatenate(tiles[2 * half:2 * half + 2], axis=0)
            return carry

        lax.fori_loop(0, n_seq // SEQ_UNROLL, seq_group, 0)
        peers = pl.ds(0, (n_sp - 1) * 16)
        rs_all = pltpu.make_async_remote_copy(
            src_ref=send.at[layer, peers, :], dst_ref=recv.at[layer, peers, :],
            send_sem=rs_ss.at[layer], recv_sem=rs_rs.at[layer], device_id=at_sp(me), device_id_type=MESH)
        rs_all.wait_recv()

        stats = jnp.concatenate([recv[layer, pl.ds(8 * t + heads, n_sp, stride=16), :] for t in range(2)], axis=0)
        stats = jnp.transpose(stats)
        tops, totals = stats[0:8], stats[LANES // 2:LANES // 2 + 8]
        for t in range(2):
            top_t = tops[:, t * n_sp:(t + 1) * n_sp]
            weight = jnp.exp(top_t - jnp.max(top_t, axis=-1, keepdims=True))
            denom = jnp.sum(weight * totals[:, t * n_sp:(t + 1) * n_sp], axis=-1, keepdims=True)
            numer = [jnp.zeros((8, LANES), F32) for _ in range(4)]
            for src in range(n_sp):
                numer[src % 4] = numer[src % 4] + weight[:, src:src + 1] * recv[layer, src * 16 + 8 * t:src * 16 + 8 * t + 8, :]
            merged = ((numer[0] + numer[1]) + (numer[2] + numer[3])) / denom
            for h in range(heads):
                pad_a[t:t + 1, h * LANES:(h + 1) * LANES] = merged[h:h + 1, :]

        wo_copy(layer).wait()
        part = dot(pad_a[...].astype(BF16), wo_v[...])[0:8]
        if layer + 1 < n_layers:
            wo_copy(layer + 1).start()
        u1 = (res[0:8, :] + exchange(layer, 0, part)).astype(BF16).astype(F32)
        h2 = rms_norm(jnp.concatenate([u1, jnp.zeros_like(u1)], axis=0), gm[layer:layer + 1, :])

        def gate_up(c, size):
            cols_copy(wg, wg_v, g_sem, layer, c, size).wait()
            cols_copy(wu, wu_v, u_sem, layer, c, size).wait()
            cols = pl.ds(pl.multiple_of(c * chunk, LANES), size)
            gate = dot(h2, wg_v[:, cols])
            up = dot(h2, wu_v[:, cols])
            g_v[:, cols] = (jax.nn.silu(gate) * up).astype(BF16)
            if layer + 1 < n_layers:
                cols_copy(wg, wg_v, g_sem, layer + 1, c, size).start()
                cols_copy(wu, wu_v, u_sem, layer + 1, c, size).start()

        def down(c, size):
            rows_copy(layer, c, size).wait()
            rows = pl.ds(pl.multiple_of(c * chunk, LANES), size)
            acc[...] += dot(g_v[:, rows], wd_v[rows, :])
            if layer + 1 < n_layers:
                rows_copy(layer + 1, c, size).start()

        def loop_of(piece):
            def step(c, carry):
                piece(c, chunk)
                return carry

            lax.fori_loop(0, n_full, step, 0)
            if tail:
                piece(n_full, tail)

        loop_of(gate_up)
        acc[...] = jnp.zeros_like(acc)
        loop_of(down)
        u2 = (u1 + exchange(layer, 1, acc[0:8, :])).astype(BF16).astype(F32)
        res[0:8, :] = u2

        row = jnp.where(core == 0, u2[0:1], u2[1:2])
        for j in range(blocks):
            ag[layer, j:j + 1, :] = row[:, j * LANES:(j + 1) * LANES]
        home = pl.ds(pl.multiple_of(me * 16, 16), blocks)
        ubuf[layer, core, home, :] = jnp.concatenate([row[:, j * LANES:(j + 1) * LANES] for j in range(blocks)], axis=0)

        def share(i, carry):
            dst = lax.rem(me + lax.rem(i + n_sp // 2, n_sp), n_sp)

            @pl.when(dst != me)
            def _():
                pltpu.make_async_remote_copy(
                    src_ref=ag.at[layer], dst_ref=ubuf.at[layer, core, home, :],
                    send_sem=ag_ss.at[layer], recv_sem=ag_rs.at[layer],
                    device_id=at_sp(dst), device_id_type=MESH).start()

            return carry

        lax.fori_loop(0, n_sp, share, 0)
        got = pl.ds(0, (n_sp - 1) * blocks)
        ag_all = pltpu.make_async_remote_copy(
            src_ref=ubuf.at[layer, core, got, :], dst_ref=ubuf.at[layer, core, got, :],
            send_sem=ag_ss.at[layer], recv_sem=ag_rs.at[layer], device_id=at_sp(me), device_id_type=MESH)
        ag_all.wait_recv()
        swap = pltpu.make_async_remote_copy(
            src_ref=ubuf.at[layer, core], dst_ref=ubuf.at[layer, core], send_sem=dd_ss.at[layer], recv_sem=dd_rs.at[layer],
            device_id={'tp': other}, device_id_type=MESH)
        swap.start()
        swap.wait()
        rs_all.wait_send()
        ag_all.wait_send()
        if layer + 1 < n_layers:
            for c in range(2):
                for j in range(blocks):
                    u3[j, pl.ds(c, n_sp, stride=2), :] = ubuf[layer, c, pl.ds(j, n_sp, stride=16), :]
        else:
            for s in range(n_steps):
                for j in range(blocks):
                    rows = pl.ds((s // 2) * 16 + j, n_seq, stride=32)
                    out[s, :, j * LANES:(j + 1) * LANES] = ubuf[layer, s % 2, rows, :].astype(BF16)


def solution(mesh):
    sp_size = mesh.shape['sp']
    dims = (4, 4, 4) if sp_size == 64 else (2, 2, 2)

    def local_fn(tok_emb, lengths, key_cache, val_cache, gain_attn, gain_mlp, w_query, w_key, w_value, w_out, w_gate, w_up, w_down):
        n_steps, n_seq, d_model = tok_emb.shape
        n_layers, _, loc_len, _, head_dim = key_cache.shape
        heads = w_query.shape[2] // head_dim
        ff = w_gate.shape[2]
        n_tok = n_steps * n_seq
        my_sp = lax.axis_index('sp')
        cur_pos = lengths[:, None] + jnp.arange(n_steps)[None, :]
        flat_pos = cur_pos.reshape(n_tok)
        half_dim = head_dim // 2
        inv_freq = 1.0 / (ROPE_BASE ** (jnp.arange(half_dim).astype(F32) * 2.0 / head_dim))
        angles = flat_pos.astype(F32)[:, None] * inv_freq[None, :]
        cos_h, sin_h = jnp.cos(angles), jnp.sin(angles)
        cos_a = jnp.concatenate([cos_h, cos_h], axis=-1)
        sin_a = jnp.concatenate([-sin_h, sin_h], axis=-1)
        lim = jnp.broadcast_to(jnp.floor_divide(flat_pos - my_sp, sp_size)[:, None], (n_tok, LANES)).astype(jnp.int32)
        wslot = jnp.where(cur_pos % sp_size == my_sp, cur_pos // sp_size, -1)
        slot = jnp.max(wslot, axis=1)
        wsl = jnp.broadcast_to(wslot.T[:, :, None], (n_steps, n_seq, LANES)).astype(jnp.int32)
        slot_b = jnp.broadcast_to(slot[:, None], (n_seq, LANES)).astype(jnp.int32)
        kc = key_cache.reshape(n_layers, n_seq, loc_len, head_dim)
        vc = val_cache.reshape(n_layers, n_seq, loc_len, head_dim)
        cfg = (dims, n_steps, n_layers, n_seq, heads, d_model, ff)
        blocks = d_model // LANES
        n_piece = -(-ff // min(MLP_CHUNK, ff))
        vm, hbm = pl.BlockSpec(memory_space=pltpu.VMEM), pl.BlockSpec(memory_space=pl.ANY)
        dma = pltpu.SemaphoreType.DMA
        hidden, k_new, v_new = pl.pallas_call(
            functools.partial(decode_kernel, cfg),
            out_shape=(
                jax.ShapeDtypeStruct((n_steps, n_seq, d_model), BF16),
                jax.ShapeDtypeStruct((n_layers, n_seq, LANES), F32),
                jax.ShapeDtypeStruct((n_layers, n_seq, LANES), F32),
            ),
            in_specs=[hbm] * 10 + [vm] * 7,
            out_specs=(vm, vm, vm),
            scratch_shapes=[
                pltpu.VMEM((n_steps, n_seq, d_model), BF16),
                pltpu.VMEM((n_layers, n_seq, loc_len, head_dim), BF16),
                pltpu.VMEM((n_layers, n_seq, loc_len, head_dim), BF16),
                pltpu.VMEM((d_model, (heads + 2) * LANES), BF16),
                pltpu.VMEM((heads * LANES, d_model), BF16),
                pltpu.VMEM((d_model, ff), BF16),
                pltpu.VMEM((d_model, ff), BF16),
                pltpu.VMEM((ff, d_model), BF16),
                pltpu.VMEM((blocks, n_tok, LANES), F32),
                pltpu.VMEM((8, LANES), F32),
                pltpu.VMEM((n_tok * 8, LANES), F32),
                pltpu.VMEM((n_tok * 8, LANES), jnp.int32),
                pltpu.VMEM((n_tok, LANES), F32),
                pltpu.VMEM((n_tok, LANES), F32),
                pltpu.VMEM((n_seq, LANES), F32),
                pltpu.VMEM((n_seq, LANES), F32),
                pltpu.VMEM((n_layers, n_tok * 8, LANES), F32),
                pltpu.VMEM((n_layers, n_tok * 8, LANES), F32),
                pltpu.VMEM((16, heads * LANES), F32),
                pltpu.VMEM((16, d_model), F32),
                pltpu.VMEM((16, ff), BF16),
                pltpu.VMEM((16, d_model), F32),
                pltpu.VMEM((n_layers, 2, 8, d_model), F32),
                pltpu.VMEM((n_layers, 2, 8, d_model), F32),
                pltpu.VMEM((n_layers, blocks, LANES), F32),
                pltpu.VMEM((n_layers, 2, sp_size * 16, LANES), F32),
                dma, dma((n_layers, 2)), dma((3,)), dma, dma((n_piece,)), dma((n_piece,)), dma((n_piece,)),
                dma((n_layers,)), dma((n_layers,)), dma((n_layers, 2)), dma((n_layers, 2)),
                dma((n_layers,)), dma((n_layers,)), dma((n_layers,)), dma((n_layers,)),
            ],
            compiler_params=pltpu.CompilerParams(collective_id=0, has_side_effects=True, vmem_limit_bytes=67043328),
        )(tok_emb, kc, vc, w_query, w_key, w_value, w_out, w_gate, w_up, w_down, cos_a, sin_a, lim, wsl, slot_b, gain_attn, gain_mlp)
        here = (jnp.arange(loc_len)[None, :] == slot[:, None])[None, :, :, None, None]
        new_keys = jnp.where(here, k_new.astype(BF16)[:, :, None, None, :], key_cache)
        new_vals = jnp.where(here, v_new.astype(BF16)[:, :, None, None, :], val_cache)
        return hidden, new_keys, new_vals

    cache_spec = P(None, 'dp', 'sp', 'tp', None)
    col_spec = P(None, None, 'tp')
    row_spec = P(None, 'tp', None)
    emb_spec = P(None, 'dp', None)
    return jax.shard_map(local_fn, mesh=mesh, in_specs=(emb_spec, P('dp'), cache_spec, cache_spec, P(), P(), col_spec, col_spec, col_spec, row_spec, col_spec, col_spec, row_spec), out_specs=(emb_spec, cache_spec, cache_spec), check_vma=False)
```

```python
import functools
import jax
import jax.numpy as jnp
import numpy as np
from jax import lax
from jax.experimental import pallas as pl
from jax.experimental.pallas import tpu as pltpu
from jax.sharding import PartitionSpec as P

EPS = 1e-5
ROPE_BASE = 500000.0
F32 = jnp.float32
BF16 = jnp.bfloat16
MESH = pl.DeviceIdType.MESH
LANES = 128
MLP_CHUNK = 1280
STORE_PARTS = 4


def rms_norm(x, gain):
    inv_rms = lax.rsqrt(jnp.mean(x * x, axis=-1, keepdims=True) + EPS)
    return (x * inv_rms * gain.astype(F32)).astype(BF16)


def dot(a, b):
    return jnp.dot(a, b, preferred_element_type=F32)


def sin_cos(angle):
    turns = jnp.floor(angle * 0.6366197723675814 + 0.5)
    x = ((angle - turns * 1.5703125) - turns * 4.837512969970703125e-4) - turns * 7.54978995489188216e-8
    z = x * x
    sin_x = x + x * z * ((-1.9515295891e-4 * z + 8.3321608736e-3) * z - 1.6666654611e-1)
    cos_x = 1.0 - 0.5 * z + z * z * ((2.443315711809948e-5 * z - 1.388731625493765e-3) * z + 4.166664568298827e-2)
    quarter = turns - 4.0 * jnp.floor(turns * 0.25)
    odd = (quarter == 1.0) | (quarter == 3.0)
    sin_a = jnp.where(odd, cos_x, sin_x)
    cos_a = jnp.where(odd, sin_x, cos_x)
    sin_a = jnp.where(quarter >= 2.0, -sin_a, sin_a)
    cos_a = jnp.where((quarter == 1.0) | (quarter == 2.0), -cos_a, cos_a)
    return sin_a, cos_a


def decode_kernel(cfg, emb, kc, vc, wq, wk, wv, wo, wg, wu, wd, len_ref, freq_ref, ga, gm,
                  out, ksel_out, vsel_out,
                  emb_v, k_v, v_v, wqkv_v, wo_v, wg_v, wu_v, wd_v, u3, qs, limr, sc, wts, ktok, vtok, ksel, vsel, cos_ref, sin_ref, step_sel, slot_ref,
                  send, recv, pad_a, res, g_v, acc, xs, xr, ag, ubuf,
                  in_sem, kv_sem, qkv_sem, wo_sem, g_sem, u_sem, d_sem,
                  rs_ss, rs_rs, x_ss, x_rs, ag_ss, ag_rs, dd_ss, dd_rs):
    dims, n_steps, n_layers, n_seq, heads, d_model, ff = cfg
    nz, ny, nx = dims
    n_sp = nz * ny * nx
    n_tok = n_steps * n_seq
    blocks = d_model // LANES
    q_cols = heads * LANES
    chunk = min(MLP_CHUNK, ff)
    n_full, tail = ff // chunk, ff % chunk
    me = lax.axis_index('sp')
    core = lax.axis_index('tp')
    other = 1 - core

    def at_sp(dst):
        return {'sp': dst}

    scopes = []

    def mark(name):
        if scopes:
            scopes.pop().__exit__(None, None, None)
        if name:
            scope = jax.named_scope(name)
            scope.__enter__()
            scopes.append(scope)

    mark('start')
    barrier = pltpu.get_barrier_semaphore()

    def hello(i, carry):
        peer = lax.rem(me + i, n_sp)
        pl.semaphore_signal(barrier, inc=1, device_id=at_sp(peer), device_id_type=MESH)
        return carry

    lax.fori_loop(1, n_sp, hello, 0)
    pl.semaphore_signal(barrier, inc=1, device_id={'tp': other}, device_id_type=MESH)

    def qkv_copies(layer):
        return [
            pltpu.make_async_copy(wq.at[layer], wqkv_v.at[:, pl.ds(0, q_cols)], qkv_sem.at[0]),
            pltpu.make_async_copy(wk.at[layer], wqkv_v.at[:, pl.ds(q_cols, LANES)], qkv_sem.at[1]),
            pltpu.make_async_copy(wv.at[layer], wqkv_v.at[:, pl.ds(q_cols + LANES, LANES)], qkv_sem.at[2]),
        ]

    def kv_copies(layer):
        return [
            pltpu.make_async_copy(kc.at[layer], k_v.at[layer], kv_sem.at[layer, 0]),
            pltpu.make_async_copy(vc.at[layer], v_v.at[layer], kv_sem.at[layer, 1]),
        ]

    def wo_copy(layer):
        return pltpu.make_async_copy(wo.at[layer], wo_v, wo_sem)

    def cols_copy(hbm, vmem, sem, layer, c, size):
        cols = pl.ds(pl.multiple_of(c * chunk, LANES), size)
        return pltpu.make_async_copy(hbm.at[layer, :, cols], vmem.at[:, cols], sem.at[c])

    def rows_copy(layer, c, size):
        rows = pl.ds(pl.multiple_of(c * chunk, LANES), size)
        return pltpu.make_async_copy(wd.at[layer, rows, :], wd_v.at[rows, :], d_sem.at[c])

    pieces = [(c, chunk) for c in range(n_full)] + ([(n_full, tail)] if tail else [])

    emb_copy = pltpu.make_async_copy(emb, emb_v, in_sem)
    emb_copy.start()
    for copy in qkv_copies(0) + kv_copies(0):
        copy.start()
    eye = lax.broadcasted_iota(jnp.int32, (n_seq, n_seq), 0) == lax.broadcasted_iota(jnp.int32, (n_seq, n_seq), 1)
    lens = jnp.sum(jnp.where(eye, len_ref[...].astype(F32), 0.0), axis=-1, keepdims=True)
    lens = jnp.broadcast_to(lens, (n_seq, LANES))
    me_f = me.astype(F32)
    sel = jnp.full((n_seq, LANES), -1.0, F32)
    for s in range(n_steps):
        pos = lens + float(s)
        row = jnp.floor(pos * (1.0 / n_sp))
        col = pos - row * n_sp
        sel = jnp.where(col == me_f, float(s), sel)
        if s == 0:
            cached = jnp.where(col <= me_f, row - 1.0, row)
            slot_ref[...] = cached + 1.0
        lim = jnp.where(sel >= 0.0, cached + 1.0, cached)
        for r in range(8):
            limr[pl.ds(s * 8 + r, n_seq, stride=8 * n_steps), :] = lim
        sin_a, cos_a = sin_cos(pos * freq_ref[...])
        first = lax.broadcasted_iota(jnp.int32, (n_seq, LANES), 1) < LANES // 2
        sin_ref[pl.ds(s, n_seq, stride=n_steps), :] = jnp.where(first, -sin_a, sin_a)
        cos_ref[pl.ds(s, n_seq, stride=n_steps), :] = cos_a
    slot_ref[...] = jnp.where(sel >= 0.0, slot_ref[...], -1.0)
    step_sel[...] = sel
    zeros = jnp.zeros((n_tok, LANES), F32)
    for r in range(heads, 8):
        qs[pl.ds(r, n_tok, stride=8), :] = zeros
    pad_a[...] = jnp.zeros_like(pad_a)
    res[...] = jnp.zeros_like(res)

    emb_copy.wait()
    for s in range(n_steps):
        for j in range(blocks):
            u3[j, pl.ds(s, n_seq, stride=n_steps), :] = emb_v[s, :, j * LANES:(j + 1) * LANES].astype(F32)
    for t in range(2):
        for j in range(blocks):
            res[t:t + 1, j * LANES:(j + 1) * LANES] = u3[j, pl.ds(2 * me + t, 1), :]

    def exchange(layer, phase, part):
        xs[layer, phase] = part
        copy = pltpu.make_async_remote_copy(
            src_ref=xs.at[layer, phase], dst_ref=xr.at[layer, phase], send_sem=x_ss.at[layer, phase], recv_sem=x_rs.at[layer, phase],
            device_id={'tp': other}, device_id_type=MESH)
        copy.start()
        copy.wait()
        return part + xr[layer, phase]

    for layer in range(n_layers):
        mark('qkv')
        x = jnp.concatenate([u3[j] for j in range(blocks)], axis=-1)
        normed = rms_norm(x, ga[layer:layer + 1, :])
        for copy in qkv_copies(layer):
            copy.wait()
        if layer == 0:
            wo_copy(0).start()
            for c, size in pieces:
                cols_copy(wg, wg_v, g_sem, 0, c, size).start()
                cols_copy(wu, wu_v, u_sem, 0, c, size).start()
            for c, size in pieces:
                rows_copy(0, c, size).start()
            for copy in kv_copies(1):
                copy.start()
        qkv = dot(normed, wqkv_v[...])
        if layer + 1 < n_layers:
            for copy in qkv_copies(layer + 1):
                copy.start()
        cos_a, sin_a = cos_ref[...], sin_ref[...]

        def rotate(vec):
            return (vec * cos_a + pltpu.roll(vec, LANES // 2, 1) * sin_a).astype(BF16).astype(F32)

        for h in range(heads):
            qs[pl.ds(h, n_tok, stride=8), :] = rotate(qkv[:, h * LANES:(h + 1) * LANES])
        ktok[...] = rotate(qkv[:, q_cols:q_cols + LANES])
        vtok[...] = qkv[:, q_cols + LANES:q_cols + 2 * LANES].astype(BF16).astype(F32)
        k_mine = jnp.zeros((n_seq, LANES), F32)
        v_mine = jnp.zeros((n_seq, LANES), F32)
        for s in range(n_steps):
            mine = step_sel[...] == float(s)
            k_mine = jnp.where(mine, ktok[pl.ds(s, n_seq, stride=n_steps), :], k_mine)
            v_mine = jnp.where(mine, vtok[pl.ds(s, n_seq, stride=n_steps), :], v_mine)
        ksel[...] = k_mine
        vsel[...] = v_mine
        ksel_out[layer] = k_mine
        vsel_out[layer] = v_mine
        mark('kvwait')
        if layer == 0:
            pl.semaphore_wait(barrier, n_sp)
        for copy in kv_copies(layer):
            copy.wait()

        seq_rows = 8 * n_steps
        slot_ids = lax.broadcasted_iota(jnp.int32, (LANES, LANES), 0).astype(F32).astype(BF16)

        def with_new(cache, new, b):
            here = slot_ids == jnp.broadcast_to(slot_ref[pl.ds(b, 1), :].astype(BF16), (LANES, LANES))
            return jnp.where(here, jnp.broadcast_to(new[pl.ds(b, 1), :].astype(BF16), (LANES, LANES)), cache[layer, b])

        mark('scores')
        for b in range(n_seq):
            rows = pl.ds(b * seq_rows, seq_rows)
            sc[rows, :] = lax.dot_general(qs[rows, :].astype(BF16), with_new(k_v, ksel, b), (((1,), (1,)), ((), ())),
                                          preferred_element_type=F32)
        mark('softmax')
        sub = lax.broadcasted_iota(jnp.int32, (8, LANES), 0)
        lane = lax.broadcasted_iota(jnp.int32, (8, LANES), 1)
        for b in range(n_seq):
            rows = pl.ds(b * seq_rows, seq_rows)
            valid = lax.broadcasted_iota(jnp.int32, (seq_rows, LANES), 1).astype(F32) <= limr[rows, :]
            scores = jnp.where(valid, sc[rows, :] * LANES ** -0.5, -1e30)
            top = jnp.max(scores, axis=-1, keepdims=True)
            w = jnp.exp(scores - top)
            total = jnp.sum(w, axis=-1, keepdims=True)
            wts[rows, :] = w.astype(BF16)
            for t in range(n_steps):
                part = slice(8 * t, 8 * t + 8)
                stat = jnp.where(lane == sub, top[part], jnp.where(lane == sub + LANES // 2, total[part], 0.0))
                sc[pl.ds(b * seq_rows + 8 * t, 8), :] = jnp.broadcast_to(jnp.sum(stat, axis=0, keepdims=True), (8, LANES))
        mark('values')
        home = pl.ds(pl.multiple_of(me * 16, 16), 16)
        is_stat = lax.rem(lax.broadcasted_iota(jnp.int32, (seq_rows, LANES), 0), 8) == heads
        plane = ny * nx // 2

        def plane_of(i, carry):
            first_seq = lax.rem(me // (ny * nx) + nz // 2 + i, nz) * plane
            seqs = [first_seq + lax.rem(lax.rem(me // 2, plane) + plane // 2 + k, plane) for k in range(plane)]
            parts = []
            for b in seqs:
                rows = pl.ds(pl.multiple_of(b * seq_rows, seq_rows), seq_rows)
                parts.append(jnp.where(is_stat, sc[rows, :], dot(wts[rows, :], with_new(v_v, vsel, b))))
            for b, part in zip(seqs, parts):
                send[layer, pl.ds(pl.multiple_of(b * seq_rows, seq_rows), seq_rows), :] = part
            for b in seqs:
                for half in range(2):
                    dst = 2 * b + half
                    rows = pl.ds(pl.multiple_of(dst * 16, 16), 16)

                    @pl.when(dst != me)
                    def _():
                        pltpu.make_async_remote_copy(
                            src_ref=send.at[layer, rows, :], dst_ref=recv.at[layer, home, :],
                            send_sem=rs_ss.at[layer], recv_sem=rs_rs.at[layer],
                            device_id=at_sp(dst), device_id_type=MESH).start()

            return carry

        lax.fori_loop(0, nz, plane_of, 0)
        recv[layer, home, :] = send[layer, home, :]
        peers = pl.ds(0, (n_sp - 1) * 16)
        rs_all = pltpu.make_async_remote_copy(
            src_ref=send.at[layer, peers, :], dst_ref=recv.at[layer, peers, :],
            send_sem=rs_ss.at[layer], recv_sem=rs_rs.at[layer], device_id=at_sp(me), device_id_type=MESH)
        mark('rswait')
        rs_all.wait_recv()

        mark('merge')
        stats = jnp.concatenate([recv[layer, pl.ds(8 * t + heads, n_sp, stride=16), :] for t in range(2)], axis=0)
        stats = jnp.transpose(stats)
        tops, totals = stats[0:8], stats[LANES // 2:LANES // 2 + 8]
        for t in range(2):
            top_t = tops[:, t * n_sp:(t + 1) * n_sp]
            weight = jnp.exp(top_t - jnp.max(top_t, axis=-1, keepdims=True))
            denom = jnp.sum(weight * totals[:, t * n_sp:(t + 1) * n_sp], axis=-1, keepdims=True)
            numer = [jnp.zeros((8, LANES), F32) for _ in range(4)]
            for src in range(n_sp):
                numer[src % 4] = numer[src % 4] + weight[:, src:src + 1] * recv[layer, src * 16 + 8 * t:src * 16 + 8 * t + 8, :]
            merged = ((numer[0] + numer[1]) + (numer[2] + numer[3])) / denom
            for h in range(heads):
                pad_a[t:t + 1, h * LANES:(h + 1) * LANES] = merged[h:h + 1, :]

        mark('wout')
        wo_copy(layer).wait()
        part = dot(pad_a[...].astype(BF16), wo_v[...])[0:8]
        if layer + 1 < n_layers:
            wo_copy(layer + 1).start()
        u1 = (res[0:8, :] + exchange(layer, 0, part)).astype(BF16).astype(F32)
        mark('gateup')
        h2 = rms_norm(jnp.concatenate([u1, jnp.zeros_like(u1)], axis=0), gm[layer:layer + 1, :])

        def gate_up(c, size):
            cols_copy(wg, wg_v, g_sem, layer, c, size).wait()
            cols_copy(wu, wu_v, u_sem, layer, c, size).wait()
            cols = pl.ds(pl.multiple_of(c * chunk, LANES), size)
            gate = dot(h2, wg_v[:, cols])
            up = dot(h2, wu_v[:, cols])
            g_v[:, cols] = (jax.nn.silu(gate) * up).astype(BF16)
            if layer + 1 < n_layers:
                cols_copy(wg, wg_v, g_sem, layer + 1, c, size).start()
                cols_copy(wu, wu_v, u_sem, layer + 1, c, size).start()

        def down(c, size):
            rows_copy(layer, c, size).wait()
            rows = pl.ds(pl.multiple_of(c * chunk, LANES), size)
            acc[...] += dot(g_v[:, rows], wd_v[rows, :])
            if layer + 1 < n_layers:
                rows_copy(layer + 1, c, size).start()

        def loop_of(piece):
            def step(c, carry):
                piece(c, chunk)
                return carry

            lax.fori_loop(0, n_full, step, 0)
            if tail:
                piece(n_full, tail)

        loop_of(gate_up)
        mark('down')
        acc[...] = jnp.zeros_like(acc)
        loop_of(down)
        mark('tp2')
        u2 = (u1 + exchange(layer, 1, acc[0:8, :])).astype(BF16).astype(F32)
        res[0:8, :] = u2

        mark('agsend')
        row = jnp.where(core == 0, u2[0:1], u2[1:2])
        for j in range(blocks):
            ag[layer, j:j + 1, :] = row[:, j * LANES:(j + 1) * LANES]
        home = pl.ds(pl.multiple_of(me * 16, 16), blocks)
        ubuf[layer, core, home, :] = jnp.concatenate([row[:, j * LANES:(j + 1) * LANES] for j in range(blocks)], axis=0)
        per_plane = ny * nx
        my_plane = me // per_plane
        mine_in = lax.rem(me, per_plane)
        orders = [(nz // 2 + i) % nz for i in range(nz)]
        orders = sorted(orders, key=lambda dz: -min(dz, nz - dz))
        for dz in orders:
            first = lax.rem(my_plane + dz, nz) * per_plane

            def share(i, carry):
                dst = first + lax.rem(mine_in + i, per_plane)
                pltpu.make_async_remote_copy(
                    src_ref=ag.at[layer], dst_ref=ubuf.at[layer, core, home, :],
                    send_sem=ag_ss.at[layer], recv_sem=ag_rs.at[layer, my_plane],
                    device_id=at_sp(dst), device_id_type=MESH).start()
                return carry

            lax.fori_loop(1 if dz == 0 else 0, per_plane, share, 0)
        mark('agwait')
        swaps = []
        for k, dz in enumerate(orders):
            src_plane = lax.rem(my_plane + nz - dz, nz)
            first_row = pl.multiple_of(src_plane * per_plane * 16, 16)
            got = pl.ds(first_row, (per_plane - (1 if dz == 0 else 0)) * blocks)
            pltpu.make_async_remote_copy(
                src_ref=ubuf.at[layer, core, got, :], dst_ref=ubuf.at[layer, core, got, :],
                send_sem=ag_ss.at[layer], recv_sem=ag_rs.at[layer, src_plane], device_id=at_sp(me), device_id_type=MESH).wait_recv()
            rows = pl.ds(first_row, per_plane * 16)
            swap = pltpu.make_async_remote_copy(
                src_ref=ubuf.at[layer, core, rows, :], dst_ref=ubuf.at[layer, core, rows, :],
                send_sem=dd_ss.at[layer, k], recv_sem=dd_rs.at[layer, k], device_id={'tp': other}, device_id_type=MESH)
            swap.start()
            swaps.append(swap)
        mark('swap')
        for swap in swaps:
            swap.wait()
        mark('fin')
        got = pl.ds(0, (n_sp - 1) * blocks)
        ag_all = pltpu.make_async_remote_copy(
            src_ref=ubuf.at[layer, core, got, :], dst_ref=ubuf.at[layer, core, got, :],
            send_sem=ag_ss.at[layer], recv_sem=ag_rs.at[layer, 0], device_id=at_sp(me), device_id_type=MESH)
        rs_all.wait_send()
        ag_all.wait_send()
        if layer + 1 < n_layers:
            for c in range(2):
                for j in range(blocks):
                    u3[j, pl.ds(c, n_sp, stride=2), :] = ubuf[layer, c, pl.ds(j, n_sp, stride=16), :]
        else:
            for s in range(n_steps):
                for j in range(blocks):
                    rows = pl.ds((s // 2) * 16 + j, n_seq, stride=32)
                    out[s, :, j * LANES:(j + 1) * LANES] = ubuf[layer, s % 2, rows, :].astype(BF16)

    mark(None)


def store_kernel(n_sp, n_steps, len_ref, hid, kc, vc, k_new, v_new, hid_out, kc_out, vc_out, hid_v, k_v, v_v, hid_sem, in_sem, out_sem):
    n_layers, n_seq = k_v.shape[0], k_v.shape[1]
    me = lax.axis_index('sp')
    part = n_seq // STORE_PARTS
    parts = [(layer, p, i) for layer in range(n_layers) for p in range(STORE_PARTS) for i in range(2)]
    hbm_in, vmem, hbm_out, new = (kc, vc), (k_v, v_v), (kc_out, vc_out), (k_new, v_new)

    def piece(ref, layer, p):
        return ref.at[layer, pl.ds(p * part, part)]

    def read(n):
        layer, p, i = parts[n]
        return pltpu.make_async_copy(piece(hbm_in[i], layer, p), piece(vmem[i], layer, p), in_sem.at[n])

    def write(n):
        layer, p, i = parts[n]
        return pltpu.make_async_copy(piece(vmem[i], layer, p), piece(hbm_out[i], layer, p), out_sem.at[n])

    for n in range(len(parts)):
        read(n).start()
    hid_in = pltpu.make_async_copy(hid, hid_v, hid_sem.at[0])
    hid_in.start()
    for n in range(len(parts)):
        layer, p, i = parts[n]
        read(n).wait()

        updates = []
        for b in range(p * part, p * part + part):
            length = len_ref[b]
            step = lax.rem(me - lax.rem(length, n_sp) + n_sp, n_sp)
            slot = jnp.where(step < n_steps, lax.div(length + step, n_sp), 0)
            tile = pl.ds(pl.multiple_of(lax.div(slot, 16) * 16, 16), 16)
            old = vmem[i][layer, b, tile, :]
            here = lax.broadcasted_iota(jnp.int32, old.shape, 0) == jnp.where(step < n_steps, lax.rem(slot, 16), -1)
            updates.append((b, tile, jnp.where(here, new[i][layer, b:b + 1, :], old.astype(F32)).astype(BF16)))
        for b, tile, value in updates:
            vmem[i][layer, b, tile, :] = value
        write(n).start()
    hid_in.wait()
    hid_back = pltpu.make_async_copy(hid_v, hid_out, hid_sem.at[1])
    hid_back.start()
    for n in range(len(parts)):
        write(n).wait()
    hid_back.wait()


def solution(mesh):
    sp_size = mesh.shape['sp']
    dims = (4, 4, 4) if sp_size == 64 else (2, 2, 2)

    def local_fn(tok_emb, lengths, key_cache, val_cache, gain_attn, gain_mlp, w_query, w_key, w_value, w_out, w_gate, w_up, w_down):
        n_steps, n_seq, d_model = tok_emb.shape
        n_layers, _, loc_len, _, head_dim = key_cache.shape
        heads = w_query.shape[2] // head_dim
        ff = w_gate.shape[2]
        n_tok = n_steps * n_seq
        half = np.arange(LANES) % (LANES // 2)
        freq = jnp.asarray((1.0 / ROPE_BASE ** (half * 2.0 / head_dim)).astype(np.float32)[None, :])
        kc = key_cache.reshape(n_layers, n_seq, loc_len, head_dim)
        vc = val_cache.reshape(n_layers, n_seq, loc_len, head_dim)
        cfg = (dims, n_steps, n_layers, n_seq, heads, d_model, ff)
        blocks = d_model // LANES
        n_piece = -(-ff // min(MLP_CHUNK, ff))
        vm, hbm = pl.BlockSpec(memory_space=pltpu.VMEM), pl.BlockSpec(memory_space=pl.ANY)
        dma = pltpu.SemaphoreType.DMA
        hidden, k_new, v_new = pl.pallas_call(
            functools.partial(decode_kernel, cfg),
            out_shape=(
                jax.ShapeDtypeStruct((n_steps, n_seq, d_model), BF16),
                jax.ShapeDtypeStruct((n_layers, n_seq, LANES), F32),
                jax.ShapeDtypeStruct((n_layers, n_seq, LANES), F32),
            ),
            in_specs=[hbm] * 10 + [vm] * 4,
            out_specs=(vm, vm, vm),
            scratch_shapes=[
                pltpu.VMEM((n_steps, n_seq, d_model), BF16),
                pltpu.VMEM((n_layers, n_seq, loc_len, head_dim), BF16),
                pltpu.VMEM((n_layers, n_seq, loc_len, head_dim), BF16),
                pltpu.VMEM((d_model, (heads + 2) * LANES), BF16),
                pltpu.VMEM((heads * LANES, d_model), BF16),
                pltpu.VMEM((d_model, ff), BF16),
                pltpu.VMEM((d_model, ff), BF16),
                pltpu.VMEM((ff, d_model), BF16),
                pltpu.VMEM((blocks, n_tok, LANES), F32),
                pltpu.VMEM((n_tok * 8, LANES), F32),
                pltpu.VMEM((n_tok * 8, LANES), F32),
                pltpu.VMEM((n_tok * 8, LANES), F32),
                pltpu.VMEM((n_tok * 8, LANES), BF16),
                pltpu.VMEM((n_tok, LANES), F32),
                pltpu.VMEM((n_tok, LANES), F32),
                pltpu.VMEM((n_seq, LANES), F32),
                pltpu.VMEM((n_seq, LANES), F32),
                pltpu.VMEM((n_tok, LANES), F32),
                pltpu.VMEM((n_tok, LANES), F32),
                pltpu.VMEM((n_seq, LANES), F32),
                pltpu.VMEM((n_seq, LANES), F32),
                pltpu.VMEM((n_layers, n_tok * 8, LANES), F32),
                pltpu.VMEM((n_layers, n_tok * 8, LANES), F32),
                pltpu.VMEM((16, heads * LANES), F32),
                pltpu.VMEM((16, d_model), F32),
                pltpu.VMEM((16, ff), BF16),
                pltpu.VMEM((16, d_model), F32),
                pltpu.VMEM((n_layers, 2, 8, d_model), F32),
                pltpu.VMEM((n_layers, 2, 8, d_model), F32),
                pltpu.VMEM((n_layers, blocks, LANES), F32),
                pltpu.VMEM((n_layers, 2, sp_size * 16, LANES), F32),
                dma, dma((n_layers, 2)), dma((3,)), dma, dma((n_piece,)), dma((n_piece,)), dma((n_piece,)),
                dma((n_layers,)), dma((n_layers,)), dma((n_layers, 2)), dma((n_layers, 2)),
                dma((n_layers,)), dma((n_layers, dims[0])), dma((n_layers, dims[0])), dma((n_layers, dims[0])),
            ],
            compiler_params=pltpu.CompilerParams(collective_id=0, has_side_effects=True, vmem_limit_bytes=67043328),
        )(tok_emb, kc, vc, w_query, w_key, w_value, w_out, w_gate, w_up, w_down, lengths.reshape(1, n_seq), freq, gain_attn, gain_mlp)
        smem = pl.BlockSpec(memory_space=pltpu.SMEM)
        n_parts = n_layers * STORE_PARTS * 2
        hidden, new_keys, new_vals = pl.pallas_call(
            functools.partial(store_kernel, sp_size, n_steps),
            out_shape=(
                jax.ShapeDtypeStruct((n_steps, n_seq, d_model), BF16),
                jax.ShapeDtypeStruct((n_layers, n_seq, loc_len, head_dim), BF16),
                jax.ShapeDtypeStruct((n_layers, n_seq, loc_len, head_dim), BF16),
            ),
            in_specs=[smem, hbm, hbm, hbm, vm, vm],
            out_specs=(hbm, hbm, hbm),
            scratch_shapes=[
                pltpu.VMEM((n_steps, n_seq, d_model), BF16),
                pltpu.VMEM((n_layers, n_seq, loc_len, head_dim), BF16),
                pltpu.VMEM((n_layers, n_seq, loc_len, head_dim), BF16),
                dma((2,)), dma((n_parts,)), dma((n_parts,)),
            ],
        )(lengths, hidden, kc, vc, k_new, v_new)
        return hidden, new_keys.reshape(key_cache.shape), new_vals.reshape(val_cache.shape)

    cache_spec = P(None, 'dp', 'sp', 'tp', None)
    col_spec = P(None, None, 'tp')
    row_spec = P(None, 'tp', None)
    emb_spec = P(None, 'dp', None)
    return jax.shard_map(local_fn, mesh=mesh, in_specs=(emb_spec, P('dp'), cache_spec, cache_spec, P(), P(), col_spec, col_spec, col_spec, row_spec, col_spec, col_spec, row_spec), out_specs=(emb_spec, cache_spec, cache_spec), check_vma=False)
```

```python
import functools
import jax
import jax.numpy as jnp
import numpy as np
from jax import lax
from jax.experimental import pallas as pl
from jax.experimental.pallas import tpu as pltpu
from jax.sharding import PartitionSpec as P

EPS = 1e-5
ROPE_BASE = 500000.0
F32 = jnp.float32
BF16 = jnp.bfloat16
MESH = pl.DeviceIdType.MESH
LANES = 128
MLP_CHUNK = 1280
STORE_PARTS = 4


def rms_norm(x, gain):
    inv_rms = lax.rsqrt(jnp.mean(x * x, axis=-1, keepdims=True) + EPS)
    return (x * inv_rms * gain.astype(F32)).astype(BF16)


def dot(a, b):
    return jnp.dot(a, b, preferred_element_type=F32)


def sin_cos(angle):
    turns = jnp.floor(angle * 0.6366197723675814 + 0.5)
    x = ((angle - turns * 1.5703125) - turns * 4.837512969970703125e-4) - turns * 7.54978995489188216e-8
    z = x * x
    sin_x = x + x * z * ((-1.9515295891e-4 * z + 8.3321608736e-3) * z - 1.6666654611e-1)
    cos_x = 1.0 - 0.5 * z + z * z * ((2.443315711809948e-5 * z - 1.388731625493765e-3) * z + 4.166664568298827e-2)
    quarter = turns - 4.0 * jnp.floor(turns * 0.25)
    odd = (quarter == 1.0) | (quarter == 3.0)
    sin_a = jnp.where(odd, cos_x, sin_x)
    cos_a = jnp.where(odd, sin_x, cos_x)
    sin_a = jnp.where(quarter >= 2.0, -sin_a, sin_a)
    cos_a = jnp.where((quarter == 1.0) | (quarter == 2.0), -cos_a, cos_a)
    return sin_a, cos_a


def decode_kernel(cfg, emb, kc, vc, wq, wk, wv, wo, wg, wu, wd, len_ref, freq_ref, ga, gm,
                  out, ksel_out, vsel_out,
                  emb_v, k_v, v_v, wqkv_v, wo_v, wg_v, wu_v, wd_v, u3, qs, limr, sc, ktok, vtok, ksel, vsel, cos_ref, sin_ref, step_sel, slot_ref,
                  send, recv, pad_a, res, g_v, acc, xs, xr, ag, ubuf,
                  in_sem, kv_sem, qkv_sem, wo_sem, g_sem, u_sem, d_sem,
                  rs_ss, rs_rs, x_ss, x_rs, ag_ss, ag_rs, dd_ss, dd_rs):
    dims, n_steps, n_layers, n_seq, heads, d_model, ff = cfg
    nz, ny, nx = dims
    n_sp = nz * ny * nx
    n_tok = n_steps * n_seq
    blocks = d_model // LANES
    q_cols = heads * LANES
    chunk = min(MLP_CHUNK, ff)
    n_full, tail = ff // chunk, ff % chunk
    me = lax.axis_index('sp')
    core = lax.axis_index('tp')
    other = 1 - core

    message = 2 * heads + 1
    my_z, my_y, my_x = me // (ny * nx), lax.rem(me // nx, ny), lax.rem(me, nx)

    def far_first(n):
        return sorted(range(n), key=lambda d: -min(d, n - d))

    def waves_of(sign):
        waves = []
        for i in far_first(ny):
            wave = []
            for dz in far_first(nz):
                dy = (dz + i) % ny
                row = lax.rem(my_z + sign * dz + nz, nz) * ny + lax.rem(my_y + sign * dy + ny, ny)
                wave.append((row * nx, dz == 0 and dy == 0))
            waves.append(wave)
        return waves

    waves, back_waves = waves_of(1), waves_of(-1)

    def dests(wave):
        return [first + lax.rem(my_x + dx, nx) for dx in far_first(nx) for first, own in wave if not (own and dx == 0)]

    def at_sp(dst):
        return {'sp': dst}

    scopes = []

    def mark(name):
        if scopes:
            scopes.pop().__exit__(None, None, None)
        if name:
            scope = jax.named_scope(name)
            scope.__enter__()
            scopes.append(scope)

    mark('start')
    def qkv_copies(layer):
        return [
            pltpu.make_async_copy(wq.at[layer], wqkv_v.at[:, pl.ds(0, q_cols)], qkv_sem.at[0]),
            pltpu.make_async_copy(wk.at[layer], wqkv_v.at[:, pl.ds(q_cols, LANES)], qkv_sem.at[1]),
            pltpu.make_async_copy(wv.at[layer], wqkv_v.at[:, pl.ds(q_cols + LANES, LANES)], qkv_sem.at[2]),
        ]

    def kv_copies(layer):
        return [
            pltpu.make_async_copy(kc.at[layer], k_v.at[layer], kv_sem.at[layer, 0]),
            pltpu.make_async_copy(vc.at[layer], v_v.at[layer], kv_sem.at[layer, 1]),
        ]

    def wo_copy(layer):
        return pltpu.make_async_copy(wo.at[layer], wo_v, wo_sem)

    def cols_copy(hbm, vmem, sem, layer, c, size):
        cols = pl.ds(pl.multiple_of(c * chunk, LANES), size)
        return pltpu.make_async_copy(hbm.at[layer, :, cols], vmem.at[:, cols], sem.at[c])

    def rows_copy(layer, c, size):
        rows = pl.ds(pl.multiple_of(c * chunk, LANES), size)
        return pltpu.make_async_copy(wd.at[layer, rows, :], wd_v.at[rows, :], d_sem.at[c])

    pieces = [(c, chunk) for c in range(n_full)] + ([(n_full, tail)] if tail else [])

    emb_copy = pltpu.make_async_copy(emb, emb_v, in_sem)
    emb_copy.start()
    for copy in qkv_copies(0) + kv_copies(0):
        copy.start()
    barrier = pltpu.get_barrier_semaphore()

    def hello(i, carry):
        peer = lax.rem(me + i, n_sp)
        pl.semaphore_signal(barrier, inc=1, device_id=at_sp(peer), device_id_type=MESH)
        return carry

    lax.fori_loop(1, n_sp, hello, 0)
    pl.semaphore_signal(barrier, inc=1, device_id={'tp': other}, device_id_type=MESH)

    eye = lax.broadcasted_iota(jnp.int32, (n_seq, n_seq), 0) == lax.broadcasted_iota(jnp.int32, (n_seq, n_seq), 1)
    lens = jnp.sum(jnp.where(eye, len_ref[...].astype(F32), 0.0), axis=-1, keepdims=True)
    lens = jnp.broadcast_to(lens, (n_seq, LANES))
    me_f = me.astype(F32)
    sel = jnp.full((n_seq, LANES), -1.0, F32)
    for s in range(n_steps):
        pos = lens + float(s)
        row = jnp.floor(pos * (1.0 / n_sp))
        col = pos - row * n_sp
        sel = jnp.where(col == me_f, float(s), sel)
        if s == 0:
            cached = jnp.where(col <= me_f, row - 1.0, row)
            slot_ref[...] = cached + 1.0
        lim = jnp.where(sel >= 0.0, cached + 1.0, cached)
        for h in range(heads):
            limr[pl.ds(s // 2 * 16 + s % 2 * heads + h, n_seq, stride=32), :] = lim
        sin_a, cos_a = sin_cos(pos * freq_ref[...])
        first = lax.broadcasted_iota(jnp.int32, (n_seq, LANES), 1) < LANES // 2
        sin_ref[pl.ds(s, n_seq, stride=n_steps), :] = jnp.where(first, -sin_a, sin_a)
        cos_ref[pl.ds(s, n_seq, stride=n_steps), :] = cos_a
    slot_ref[...] = jnp.where(sel >= 0.0, slot_ref[...], -1.0)
    step_sel[...] = sel
    zeros = jnp.zeros((n_sp, LANES), F32)
    for r in range(2 * heads, 16):
        qs[pl.ds(r, n_sp, stride=16), :] = zeros
        limr[pl.ds(r, n_sp, stride=16), :] = zeros
    pad_a[...] = jnp.zeros_like(pad_a)
    res[...] = jnp.zeros_like(res)

    emb_copy.wait()
    for s in range(n_steps):
        for j in range(blocks):
            u3[j, pl.ds(s, n_seq, stride=n_steps), :] = emb_v[s, :, j * LANES:(j + 1) * LANES].astype(F32)
    for t in range(2):
        for j in range(blocks):
            res[t:t + 1, j * LANES:(j + 1) * LANES] = u3[j, pl.ds(2 * me + t, 1), :]

    def exchange(layer, phase, part):
        xs[layer, phase] = part
        copy = pltpu.make_async_remote_copy(
            src_ref=xs.at[layer, phase], dst_ref=xr.at[layer, phase], send_sem=x_ss.at[layer, phase], recv_sem=x_rs.at[layer, phase],
            device_id={'tp': other}, device_id_type=MESH)
        copy.start()
        copy.wait()
        return part + xr[layer, phase]

    for layer in range(n_layers):
        mark('qkv')
        x = jnp.concatenate([u3[j] for j in range(blocks)], axis=-1)
        normed = rms_norm(x, ga[layer:layer + 1, :])
        for copy in qkv_copies(layer):
            copy.wait()
        if layer == 0:
            wo_copy(0).start()
            for c, size in pieces:
                cols_copy(wg, wg_v, g_sem, 0, c, size).start()
                cols_copy(wu, wu_v, u_sem, 0, c, size).start()
            for c, size in pieces:
                rows_copy(0, c, size).start()
            for copy in kv_copies(1):
                copy.start()
        qkv = dot(normed, wqkv_v[...])
        if layer + 1 < n_layers:
            for copy in qkv_copies(layer + 1):
                copy.start()
        cos_a, sin_a = cos_ref[...], sin_ref[...]

        def rotate(vec):
            return (vec * cos_a + pltpu.roll(vec, LANES // 2, 1) * sin_a).astype(BF16).astype(F32)

        for h in range(heads):
            sc[pl.ds(h * n_tok, n_tok), :] = rotate(qkv[:, h * LANES:(h + 1) * LANES])
        for h in range(heads):
            for t in range(2):
                qs[pl.ds(t * heads + h, n_sp, stride=16), :] = sc[pl.ds(h * n_tok + t, n_sp, stride=2), :]
        ktok[...] = rotate(qkv[:, q_cols:q_cols + LANES])
        vtok[...] = qkv[:, q_cols + LANES:q_cols + 2 * LANES].astype(BF16).astype(F32)
        k_mine = jnp.zeros((n_seq, LANES), F32)
        v_mine = jnp.zeros((n_seq, LANES), F32)
        for s in range(n_steps):
            mine = step_sel[...] == float(s)
            k_mine = jnp.where(mine, ktok[pl.ds(s, n_seq, stride=n_steps), :], k_mine)
            v_mine = jnp.where(mine, vtok[pl.ds(s, n_seq, stride=n_steps), :], v_mine)
        ksel[...] = k_mine
        vsel[...] = v_mine
        ksel_out[layer] = k_mine
        vsel_out[layer] = v_mine
        mark('kvwait')
        if layer == 0:
            pl.semaphore_wait(barrier, n_sp)
        for copy in kv_copies(layer):
            copy.wait()

        seq_rows = 8 * n_steps
        slot_ids = lax.broadcasted_iota(jnp.int32, (LANES, LANES), 0).astype(F32).astype(BF16)

        def with_new(cache, new, b):
            here = slot_ids == jnp.broadcast_to(slot_ref[pl.ds(b, 1), :].astype(BF16), (LANES, LANES))
            return jnp.where(here, jnp.broadcast_to(new[pl.ds(b, 1), :].astype(BF16), (LANES, LANES)), cache[layer, b])

        mark('scores')
        for b in range(n_seq):
            rows = pl.ds(b * seq_rows, seq_rows)
            sc[rows, :] = lax.dot_general(qs[rows, :].astype(BF16), with_new(k_v, ksel, b), (((1,), (1,)), ((), ())),
                                          preferred_element_type=F32)
        mark('values')
        sub = lax.broadcasted_iota(jnp.int32, (16, LANES), 0)
        lane = lax.broadcasted_iota(jnp.int32, (16, LANES), 1)
        home = pl.ds(pl.multiple_of(me * 16, 16), message)

        def partials(b):
            rows = pl.ds(pl.multiple_of(b * seq_rows, seq_rows), seq_rows)
            valid = lax.broadcasted_iota(jnp.int32, (seq_rows, LANES), 1).astype(F32) <= limr[rows, :]
            scores = jnp.where(valid, sc[rows, :] * LANES ** -0.5, -1e30)
            top = jnp.max(scores, axis=-1, keepdims=True)
            w = jnp.exp(scores - top)
            total = jnp.sum(w, axis=-1, keepdims=True)
            o = dot(w.astype(BF16), with_new(v_v, vsel, b))
            halves = []
            for half in range(2):
                part = slice(16 * half, 16 * half + 16)
                stat = jnp.where(lane == sub, top[part], jnp.where(lane == sub + LANES // 2, total[part], 0.0))
                halves.append(jnp.where(sub == 2 * heads, jnp.sum(stat, axis=0, keepdims=True), o[part]))
            return rows, jnp.concatenate(halves, axis=0)

        for wave in waves:
            done = [partials(first // 2 + k) for first, _ in wave for k in range(nx // 2)]
            for rows, part in done:
                send[layer, rows, :] = part
            for dst in dests(wave):
                pltpu.make_async_remote_copy(
                    src_ref=send.at[layer, pl.ds(pl.multiple_of(dst * 16, 16), message), :], dst_ref=recv.at[layer, home, :],
                    send_sem=rs_ss.at[layer], recv_sem=rs_rs.at[layer], device_id=at_sp(dst), device_id_type=MESH).start()
        recv[layer, home, :] = send[layer, home, :]
        peers = pl.ds(0, (n_sp - 1) * message)
        rs_all = pltpu.make_async_remote_copy(
            src_ref=send.at[layer, peers, :], dst_ref=recv.at[layer, peers, :],
            send_sem=rs_ss.at[layer], recv_sem=rs_rs.at[layer], device_id=at_sp(me), device_id_type=MESH)
        mark('rswait')
        rs_all.wait_recv()

        mark('merge')
        stats = jnp.transpose(recv[layer, pl.ds(2 * heads, n_sp, stride=16), :])
        tops, totals = stats[0:16], stats[LANES // 2:LANES // 2 + 16]
        weight = jnp.exp(tops - jnp.max(tops, axis=-1, keepdims=True))
        denom = jnp.sum(weight * totals, axis=-1, keepdims=True)
        numer = [jnp.zeros((16, LANES), F32) for _ in range(4)]
        for src in range(n_sp):
            numer[src % 4] = numer[src % 4] + weight[:, src:src + 1] * recv[layer, src * 16:src * 16 + 16, :]
        merged = ((numer[0] + numer[1]) + (numer[2] + numer[3])) / denom
        for t in range(2):
            for h in range(heads):
                pad_a[t:t + 1, h * LANES:(h + 1) * LANES] = merged[t * heads + h:t * heads + h + 1, :]

        mark('wout')
        wo_copy(layer).wait()
        part = dot(pad_a[...].astype(BF16), wo_v[...])[0:8]
        if layer + 1 < n_layers:
            wo_copy(layer + 1).start()
        u1 = (res[0:8, :] + exchange(layer, 0, part)).astype(BF16).astype(F32)
        mark('gateup')
        h2 = rms_norm(jnp.concatenate([u1, jnp.zeros_like(u1)], axis=0), gm[layer:layer + 1, :])

        def gate_up(c, size):
            cols_copy(wg, wg_v, g_sem, layer, c, size).wait()
            cols_copy(wu, wu_v, u_sem, layer, c, size).wait()
            cols = pl.ds(pl.multiple_of(c * chunk, LANES), size)
            gate = dot(h2, wg_v[:, cols])
            up = dot(h2, wu_v[:, cols])
            g_v[:, cols] = (jax.nn.silu(gate) * up).astype(BF16)
            if layer + 1 < n_layers:
                cols_copy(wg, wg_v, g_sem, layer + 1, c, size).start()
                cols_copy(wu, wu_v, u_sem, layer + 1, c, size).start()

        def down(c, size):
            rows_copy(layer, c, size).wait()
            rows = pl.ds(pl.multiple_of(c * chunk, LANES), size)
            acc[...] += dot(g_v[:, rows], wd_v[rows, :])
            if layer + 1 < n_layers:
                rows_copy(layer + 1, c, size).start()

        def loop_of(piece):
            def step(c, carry):
                piece(c, chunk)
                return carry

            lax.fori_loop(0, n_full, step, 0)
            if tail:
                piece(n_full, tail)

        loop_of(gate_up)
        mark('down')
        acc[...] = jnp.zeros_like(acc)
        loop_of(down)
        mark('tp2')
        u2 = (u1 + exchange(layer, 1, acc[0:8, :])).astype(BF16).astype(F32)
        res[0:8, :] = u2

        mark('agsend')
        row = jnp.where(core == 0, u2[0:1], u2[1:2])
        for j in range(blocks):
            ag[layer, j:j + 1, :] = row[:, j * LANES:(j + 1) * LANES]
        home = pl.ds(pl.multiple_of(me * 16, 16), blocks)
        ubuf[layer, core, home, :] = jnp.concatenate([row[:, j * LANES:(j + 1) * LANES] for j in range(blocks)], axis=0)
        for k, wave in enumerate(waves):
            for dst in dests(wave):
                pltpu.make_async_remote_copy(
                    src_ref=ag.at[layer], dst_ref=ubuf.at[layer, core, home, :],
                    send_sem=ag_ss.at[layer], recv_sem=ag_rs.at[layer, k],
                    device_id=at_sp(dst), device_id_type=MESH).start()
        mark('agwait')
        swaps = []
        for k, wave in enumerate(back_waves):
            count = sum(nx - (1 if own else 0) for _, own in wave)
            got = pl.ds(0, count * blocks)
            pltpu.make_async_remote_copy(
                src_ref=ubuf.at[layer, core, got, :], dst_ref=ubuf.at[layer, core, got, :],
                send_sem=ag_ss.at[layer], recv_sem=ag_rs.at[layer, k], device_id=at_sp(me), device_id_type=MESH).wait_recv()
            for q, (first, _) in enumerate(wave):
                rows = pl.ds(pl.multiple_of(first * 16, 16), nx * 16)
                swap = pltpu.make_async_remote_copy(
                    src_ref=ubuf.at[layer, core, rows, :], dst_ref=ubuf.at[layer, core, rows, :],
                    send_sem=dd_ss.at[layer, k, q], recv_sem=dd_rs.at[layer, k, q], device_id={'tp': other}, device_id_type=MESH)
                swap.start()
                swaps.append(swap)
        mark('swap')
        for swap in swaps:
            swap.wait()
        mark('fin')
        got = pl.ds(0, (n_sp - 1) * blocks)
        ag_all = pltpu.make_async_remote_copy(
            src_ref=ubuf.at[layer, core, got, :], dst_ref=ubuf.at[layer, core, got, :],
            send_sem=ag_ss.at[layer], recv_sem=ag_rs.at[layer, 0], device_id=at_sp(me), device_id_type=MESH)
        rs_all.wait_send()
        ag_all.wait_send()
        if layer + 1 < n_layers:
            for c in range(2):
                for j in range(blocks):
                    u3[j, pl.ds(c, n_sp, stride=2), :] = ubuf[layer, c, pl.ds(j, n_sp, stride=16), :]
        else:
            for s in range(n_steps):
                for j in range(blocks):
                    rows = pl.ds((s // 2) * 16 + j, n_seq, stride=32)
                    out[s, :, j * LANES:(j + 1) * LANES] = ubuf[layer, s % 2, rows, :].astype(BF16)

    mark(None)


def store_kernel(n_sp, n_steps, len_ref, hid, kc, vc, k_new, v_new, hid_out, kc_out, vc_out, hid_v, k_v, v_v, hid_sem, in_sem, out_sem):
    n_layers, n_seq = k_v.shape[0], k_v.shape[1]
    me = lax.axis_index('sp')
    part = n_seq // STORE_PARTS
    parts = [(layer, p, i) for layer in range(n_layers) for p in range(STORE_PARTS) for i in range(2)]
    hbm_in, vmem, hbm_out, new = (kc, vc), (k_v, v_v), (kc_out, vc_out), (k_new, v_new)

    def piece(ref, layer, p):
        return ref.at[layer, pl.ds(p * part, part)]

    def read(n):
        layer, p, i = parts[n]
        return pltpu.make_async_copy(piece(hbm_in[i], layer, p), piece(vmem[i], layer, p), in_sem.at[n])

    def write(n):
        layer, p, i = parts[n]
        return pltpu.make_async_copy(piece(vmem[i], layer, p), piece(hbm_out[i], layer, p), out_sem.at[n])

    for n in range(len(parts)):
        read(n).start()
    hid_in = pltpu.make_async_copy(hid, hid_v, hid_sem.at[0])
    hid_in.start()
    for n in range(len(parts)):
        layer, p, i = parts[n]
        read(n).wait()

        updates = []
        for b in range(p * part, p * part + part):
            length = len_ref[b]
            step = lax.rem(me - lax.rem(length, n_sp) + n_sp, n_sp)
            slot = jnp.where(step < n_steps, lax.div(length + step, n_sp), 0)
            tile = pl.ds(pl.multiple_of(lax.div(slot, 16) * 16, 16), 16)
            old = vmem[i][layer, b, tile, :]
            here = lax.broadcasted_iota(jnp.int32, old.shape, 0) == jnp.where(step < n_steps, lax.rem(slot, 16), -1)
            updates.append((b, tile, jnp.where(here, new[i][layer, b:b + 1, :], old.astype(F32)).astype(BF16)))
        for b, tile, value in updates:
            vmem[i][layer, b, tile, :] = value
        write(n).start()
    hid_in.wait()
    hid_back = pltpu.make_async_copy(hid_v, hid_out, hid_sem.at[1])
    hid_back.start()
    for n in range(len(parts)):
        write(n).wait()
    hid_back.wait()


def solution(mesh):
    sp_size = mesh.shape['sp']
    dims = (4, 4, 4) if sp_size == 64 else (2, 2, 2)

    def local_fn(tok_emb, lengths, key_cache, val_cache, gain_attn, gain_mlp, w_query, w_key, w_value, w_out, w_gate, w_up, w_down):
        n_steps, n_seq, d_model = tok_emb.shape
        n_layers, _, loc_len, _, head_dim = key_cache.shape
        heads = w_query.shape[2] // head_dim
        ff = w_gate.shape[2]
        n_tok = n_steps * n_seq
        half = np.arange(LANES) % (LANES // 2)
        freq = jnp.asarray((1.0 / ROPE_BASE ** (half * 2.0 / head_dim)).astype(np.float32)[None, :])
        kc = key_cache.reshape(n_layers, n_seq, loc_len, head_dim)
        vc = val_cache.reshape(n_layers, n_seq, loc_len, head_dim)
        cfg = (dims, n_steps, n_layers, n_seq, heads, d_model, ff)
        blocks = d_model // LANES
        n_piece = -(-ff // min(MLP_CHUNK, ff))
        vm, hbm = pl.BlockSpec(memory_space=pltpu.VMEM), pl.BlockSpec(memory_space=pl.ANY)
        dma = pltpu.SemaphoreType.DMA
        hidden, k_new, v_new = pl.pallas_call(
            functools.partial(decode_kernel, cfg),
            out_shape=(
                jax.ShapeDtypeStruct((n_steps, n_seq, d_model), BF16),
                jax.ShapeDtypeStruct((n_layers, n_seq, LANES), F32),
                jax.ShapeDtypeStruct((n_layers, n_seq, LANES), F32),
            ),
            in_specs=[hbm] * 10 + [vm] * 4,
            out_specs=(vm, vm, vm),
            scratch_shapes=[
                pltpu.VMEM((n_steps, n_seq, d_model), BF16),
                pltpu.VMEM((n_layers, n_seq, loc_len, head_dim), BF16),
                pltpu.VMEM((n_layers, n_seq, loc_len, head_dim), BF16),
                pltpu.VMEM((d_model, (heads + 2) * LANES), BF16),
                pltpu.VMEM((heads * LANES, d_model), BF16),
                pltpu.VMEM((d_model, ff), BF16),
                pltpu.VMEM((d_model, ff), BF16),
                pltpu.VMEM((ff, d_model), BF16),
                pltpu.VMEM((blocks, n_tok, LANES), F32),
                pltpu.VMEM((n_tok * 8, LANES), F32),
                pltpu.VMEM((n_tok * 8, LANES), F32),
                pltpu.VMEM((n_tok * 8, LANES), F32),
                pltpu.VMEM((n_tok, LANES), F32),
                pltpu.VMEM((n_tok, LANES), F32),
                pltpu.VMEM((n_seq, LANES), F32),
                pltpu.VMEM((n_seq, LANES), F32),
                pltpu.VMEM((n_tok, LANES), F32),
                pltpu.VMEM((n_tok, LANES), F32),
                pltpu.VMEM((n_seq, LANES), F32),
                pltpu.VMEM((n_seq, LANES), F32),
                pltpu.VMEM((n_layers, n_tok * 8, LANES), F32),
                pltpu.VMEM((n_layers, n_tok * 8, LANES), F32),
                pltpu.VMEM((16, heads * LANES), F32),
                pltpu.VMEM((16, d_model), F32),
                pltpu.VMEM((16, ff), BF16),
                pltpu.VMEM((16, d_model), F32),
                pltpu.VMEM((n_layers, 2, 8, d_model), F32),
                pltpu.VMEM((n_layers, 2, 8, d_model), F32),
                pltpu.VMEM((n_layers, blocks, LANES), F32),
                pltpu.VMEM((n_layers, 2, sp_size * 16, LANES), F32),
                dma, dma((n_layers, 2)), dma((3,)), dma, dma((n_piece,)), dma((n_piece,)), dma((n_piece,)),
                dma((n_layers,)), dma((n_layers,)), dma((n_layers, 2)), dma((n_layers, 2)),
                dma((n_layers,)), dma((n_layers, dims[1])), dma((n_layers, dims[1], dims[0])), dma((n_layers, dims[1], dims[0])),
            ],
            compiler_params=pltpu.CompilerParams(collective_id=0, has_side_effects=True, vmem_limit_bytes=67043328),
        )(tok_emb, kc, vc, w_query, w_key, w_value, w_out, w_gate, w_up, w_down, lengths.reshape(1, n_seq), freq, gain_attn, gain_mlp)
        smem = pl.BlockSpec(memory_space=pltpu.SMEM)
        n_parts = n_layers * STORE_PARTS * 2
        hidden, new_keys, new_vals = pl.pallas_call(
            functools.partial(store_kernel, sp_size, n_steps),
            out_shape=(
                jax.ShapeDtypeStruct((n_steps, n_seq, d_model), BF16),
                jax.ShapeDtypeStruct((n_layers, n_seq, loc_len, head_dim), BF16),
                jax.ShapeDtypeStruct((n_layers, n_seq, loc_len, head_dim), BF16),
            ),
            in_specs=[smem, hbm, hbm, hbm, vm, vm],
            out_specs=(hbm, hbm, hbm),
            scratch_shapes=[
                pltpu.VMEM((n_steps, n_seq, d_model), BF16),
                pltpu.VMEM((n_layers, n_seq, loc_len, head_dim), BF16),
                pltpu.VMEM((n_layers, n_seq, loc_len, head_dim), BF16),
                dma((2,)), dma((n_parts,)), dma((n_parts,)),
            ],
        )(lengths, hidden, kc, vc, k_new, v_new)
        return hidden, new_keys.reshape(key_cache.shape), new_vals.reshape(val_cache.shape)

    cache_spec = P(None, 'dp', 'sp', 'tp', None)
    col_spec = P(None, None, 'tp')
    row_spec = P(None, 'tp', None)
    emb_spec = P(None, 'dp', None)
    return jax.shard_map(local_fn, mesh=mesh, in_specs=(emb_spec, P('dp'), cache_spec, cache_spec, P(), P(), col_spec, col_spec, col_spec, row_spec, col_spec, col_spec, row_spec), out_specs=(emb_spec, cache_spec, cache_spec), check_vma=False)
```

```python
import functools
import jax
import jax.numpy as jnp
import numpy as np
from jax import lax
from jax.experimental import pallas as pl
from jax.experimental.pallas import tpu as pltpu
from jax.sharding import PartitionSpec as P

EPS = 1e-5
ROPE_BASE = 500000.0
F32 = jnp.float32
BF16 = jnp.bfloat16
MESH = pl.DeviceIdType.MESH
LANES = 128
VMEM_LIMIT = 59 * 1024 * 1024
MLP_CHUNK = 1280


def rms_norm(x, gain):
    inv_rms = lax.rsqrt(jnp.mean(x * x, axis=-1, keepdims=True) + EPS)
    return (x * inv_rms * gain.astype(F32)).astype(BF16)


def dot(a, b):
    return jnp.dot(a, b, preferred_element_type=F32)


def sin_cos(angle):
    turns = jnp.floor(angle * 0.6366197723675814 + 0.5)
    x = ((angle - turns * 1.5703125) - turns * 4.837512969970703125e-4) - turns * 7.54978995489188216e-8
    z = x * x
    sin_x = x + x * z * ((-1.9515295891e-4 * z + 8.3321608736e-3) * z - 1.6666654611e-1)
    cos_x = 1.0 - 0.5 * z + z * z * ((2.443315711809948e-5 * z - 1.388731625493765e-3) * z + 4.166664568298827e-2)
    quarter = turns - 4.0 * jnp.floor(turns * 0.25)
    odd = (quarter == 1.0) | (quarter == 3.0)
    sin_a = jnp.where(odd, cos_x, sin_x)
    cos_a = jnp.where(odd, sin_x, cos_x)
    sin_a = jnp.where(quarter >= 2.0, -sin_a, sin_a)
    cos_a = jnp.where((quarter == 1.0) | (quarter == 2.0), -cos_a, cos_a)
    return sin_a, cos_a


def decode_kernel(cfg, emb, kc, vc, wq, wk, wv, wo, wg, wu, wd, len_ref, freq_ref, ga, gm,
                  bundle,
                  out, kv_new, emb_v, k_v, v_v, wqkv_v, wo_v, wg_v, wu_v, wd_v, u3, qs, limr, sc, ktok, vtok, ksel, vsel, cos_ref, sin_ref, step_sel, slot_ref,
                  send, recv, pad_a, res, g_v, acc, xs, xr, ag, ubuf,
                  out_sem, in_sem, kv_sem, qkv_sem, wo_sem, g_sem, u_sem, d_sem,
                  rs_ss, rs_rs, x_ss, x_rs, ag_ss, ag_rs, dd_ss, dd_rs):
    dims, n_steps, n_layers, n_seq, heads, d_model, ff = cfg
    nz, ny, nx = dims
    n_sp = nz * ny * nx
    n_tok = n_steps * n_seq
    blocks = d_model // LANES
    q_cols = heads * LANES
    chunk = min(MLP_CHUNK, ff)
    n_full, tail = ff // chunk, ff % chunk
    me = lax.axis_index('sp')
    core = lax.axis_index('tp')
    other = 1 - core

    message = 2 * heads + 1
    my_z, my_y, my_x = me // (ny * nx), lax.rem(me // nx, ny), lax.rem(me, nx)

    def far_first(n):
        return sorted(range(n), key=lambda d: -min(d, n - d))

    def waves_of(sign):
        offsets = [(dz, dy) for dz in far_first(nz) for dy in far_first(ny)]
        offsets = sorted(offsets, key=lambda o: -min(o[0], nz - o[0]) - min(o[1], ny - o[1]))
        rows = []
        for dz, dy in offsets:
            row = lax.rem(my_z + sign * dz + nz, nz) * ny + lax.rem(my_y + sign * dy + ny, ny)
            rows.append((row * nx, dz == 0 and dy == 0))
        return [rows[i:i + nz] for i in range(0, len(rows), nz)]

    waves, back_waves = waves_of(1), waves_of(-1)

    def dests(wave):
        return [first + lax.rem(my_x + dx, nx) for dx in far_first(nx) for first, own in wave if not (own and dx == 0)]

    def at_sp(dst):
        return {'sp': dst}

    scopes = []

    def mark(name):
        if scopes:
            scopes.pop().__exit__(None, None, None)
        if name:
            scope = jax.named_scope(name)
            scope.__enter__()
            scopes.append(scope)

    mark('start')
    def qkv_copies(layer):
        return [
            pltpu.make_async_copy(wq.at[layer], wqkv_v.at[:, pl.ds(0, q_cols)], qkv_sem.at[0]),
            pltpu.make_async_copy(wk.at[layer], wqkv_v.at[:, pl.ds(q_cols, LANES)], qkv_sem.at[1]),
            pltpu.make_async_copy(wv.at[layer], wqkv_v.at[:, pl.ds(q_cols + LANES, LANES)], qkv_sem.at[2]),
        ]

    def kv_copies(layer):
        return [
            pltpu.make_async_copy(kc.at[layer], k_v.at[layer], kv_sem.at[layer, 0]),
            pltpu.make_async_copy(vc.at[layer], v_v.at[layer], kv_sem.at[layer, 1]),
        ]

    def wo_copy(layer):
        return pltpu.make_async_copy(wo.at[layer], wo_v, wo_sem)

    def cols_copy(hbm, vmem, sem, layer, c, size):
        cols = pl.ds(pl.multiple_of(c * chunk, LANES), size)
        return pltpu.make_async_copy(hbm.at[layer, :, cols], vmem.at[:, cols], sem.at[c])

    def rows_copy(layer, c, size):
        rows = pl.ds(pl.multiple_of(c * chunk, LANES), size)
        return pltpu.make_async_copy(wd.at[layer, rows, :], wd_v.at[rows, :], d_sem.at[c])

    pieces = [(c, chunk) for c in range(n_full)] + ([(n_full, tail)] if tail else [])

    emb_copy = pltpu.make_async_copy(emb, emb_v, in_sem)
    emb_copy.start()
    for copy in qkv_copies(0) + kv_copies(0):
        copy.start()
    barrier = pltpu.get_barrier_semaphore()

    for wave in waves:
        for dst in dests(wave):
            pl.semaphore_signal(barrier, inc=1, device_id=at_sp(dst), device_id_type=MESH)
    pl.semaphore_signal(barrier, inc=1, device_id={'tp': other}, device_id_type=MESH)

    eye = lax.broadcasted_iota(jnp.int32, (n_seq, n_seq), 0) == lax.broadcasted_iota(jnp.int32, (n_seq, n_seq), 1)
    lens = jnp.sum(jnp.where(eye, len_ref[...].astype(F32), 0.0), axis=-1, keepdims=True)
    lens = jnp.broadcast_to(lens, (n_seq, LANES))
    me_f = me.astype(F32)
    sel = jnp.full((n_seq, LANES), -1.0, F32)
    for s in range(n_steps):
        pos = lens + float(s)
        row = jnp.floor(pos * (1.0 / n_sp))
        col = pos - row * n_sp
        sel = jnp.where(col == me_f, float(s), sel)
        if s == 0:
            cached = jnp.where(col <= me_f, row - 1.0, row)
            slot_ref[...] = cached + 1.0
        lim = jnp.where(sel >= 0.0, cached + 1.0, cached)
        for h in range(heads):
            limr[pl.ds(s // 2 * 16 + s % 2 * heads + h, n_seq, stride=32), :] = lim
        sin_a, cos_a = sin_cos(pos * freq_ref[...])
        first = lax.broadcasted_iota(jnp.int32, (n_seq, LANES), 1) < LANES // 2
        sin_ref[pl.ds(s, n_seq, stride=n_steps), :] = jnp.where(first, -sin_a, sin_a)
        cos_ref[pl.ds(s, n_seq, stride=n_steps), :] = cos_a
    slot_ref[...] = jnp.where(sel >= 0.0, slot_ref[...], -1.0)
    step_sel[...] = sel
    zeros = jnp.zeros((n_sp, LANES), F32)
    for r in range(2 * heads, 16):
        qs[pl.ds(r, n_sp, stride=16), :] = zeros
        limr[pl.ds(r, n_sp, stride=16), :] = zeros
    pad_a[...] = jnp.zeros_like(pad_a)
    res[...] = jnp.zeros_like(res)

    emb_copy.wait()
    for s in range(n_steps):
        for j in range(blocks):
            u3[j, pl.ds(s, n_seq, stride=n_steps), :] = emb_v[s, :, j * LANES:(j + 1) * LANES].astype(F32)
    for t in range(2):
        for j in range(blocks):
            res[t:t + 1, j * LANES:(j + 1) * LANES] = u3[j, pl.ds(2 * me + t, 1), :]

    def exchange(layer, phase, part):
        xs[layer, phase] = part
        copy = pltpu.make_async_remote_copy(
            src_ref=xs.at[layer, phase], dst_ref=xr.at[layer, phase], send_sem=x_ss.at[layer, phase], recv_sem=x_rs.at[layer, phase],
            device_id={'tp': other}, device_id_type=MESH)
        copy.start()
        copy.wait()
        return part + xr[layer, phase]

    for layer in range(n_layers):
        mark('qkv')
        x = jnp.concatenate([u3[j] for j in range(blocks)], axis=-1)
        normed = rms_norm(x, ga[layer:layer + 1, :])
        for copy in qkv_copies(layer):
            copy.wait()
        if layer == 0:
            wo_copy(0).start()
            for c, size in pieces:
                cols_copy(wg, wg_v, g_sem, 0, c, size).start()
                cols_copy(wu, wu_v, u_sem, 0, c, size).start()
            for c, size in pieces:
                rows_copy(0, c, size).start()
            for copy in kv_copies(1):
                copy.start()
        qkv = dot(normed, wqkv_v[...])
        if layer + 1 < n_layers:
            for copy in qkv_copies(layer + 1):
                copy.start()
        cos_a, sin_a = cos_ref[...], sin_ref[...]

        def rotate(vec):
            return (vec * cos_a + pltpu.roll(vec, LANES // 2, 1) * sin_a).astype(BF16).astype(F32)

        for h in range(heads):
            sc[pl.ds(h * n_tok, n_tok), :] = rotate(qkv[:, h * LANES:(h + 1) * LANES])
        for h in range(heads):
            for t in range(2):
                qs[pl.ds(t * heads + h, n_sp, stride=16), :] = sc[pl.ds(h * n_tok + t, n_sp, stride=2), :]
        ktok[...] = rotate(qkv[:, q_cols:q_cols + LANES])
        vtok[...] = qkv[:, q_cols + LANES:q_cols + 2 * LANES].astype(BF16).astype(F32)
        k_mine = jnp.zeros((n_seq, LANES), F32)
        v_mine = jnp.zeros((n_seq, LANES), F32)
        for s in range(n_steps):
            mine = step_sel[...] == float(s)
            k_mine = jnp.where(mine, ktok[pl.ds(s, n_seq, stride=n_steps), :], k_mine)
            v_mine = jnp.where(mine, vtok[pl.ds(s, n_seq, stride=n_steps), :], v_mine)
        ksel[...] = k_mine
        vsel[...] = v_mine
        kv_new[layer, 0] = k_mine.astype(BF16)
        kv_new[layer, 1] = v_mine.astype(BF16)
        mark('kvwait')
        for copy in kv_copies(layer):
            copy.wait()

        seq_rows = 8 * n_steps
        slot_ids = lax.broadcasted_iota(jnp.int32, (LANES, LANES), 0).astype(F32).astype(BF16)

        def with_new(cache, new, b):
            here = slot_ids == jnp.broadcast_to(slot_ref[pl.ds(b, 1), :].astype(BF16), (LANES, LANES))
            return jnp.where(here, jnp.broadcast_to(new[pl.ds(b, 1), :].astype(BF16), (LANES, LANES)), cache[layer, b])

        stored = [
            pltpu.make_async_copy(kv_new.at[layer, i], bundle.at[n_steps + 2 * layer + i, :, pl.ds(0, LANES)], out_sem.at[2 * layer + i])
            for i in range(2)
        ]
        for copy in stored:
            copy.start()

        mark('scores')
        for b in range(n_seq):
            rows = pl.ds(b * seq_rows, seq_rows)
            sc[rows, :] = lax.dot_general(qs[rows, :].astype(BF16), with_new(k_v, ksel, b), (((1,), (1,)), ((), ())),
                                          preferred_element_type=F32)
        mark('values')
        sub = lax.broadcasted_iota(jnp.int32, (16, LANES), 0)
        lane = lax.broadcasted_iota(jnp.int32, (16, LANES), 1)
        home = pl.ds(pl.multiple_of(me * 16, 16), message)

        def partials(b):
            rows = pl.ds(pl.multiple_of(b * seq_rows, seq_rows), seq_rows)
            valid = lax.broadcasted_iota(jnp.int32, (seq_rows, LANES), 1).astype(F32) <= limr[rows, :]
            scores = jnp.where(valid, sc[rows, :] * LANES ** -0.5, -1e30)
            top = jnp.max(scores, axis=-1, keepdims=True)
            w = jnp.exp(scores - top)
            total = jnp.sum(w, axis=-1, keepdims=True)
            o = dot(w.astype(BF16), with_new(v_v, vsel, b))
            halves = []
            for half in range(2):
                part = slice(16 * half, 16 * half + 16)
                stat = jnp.where(lane == sub, top[part], jnp.where(lane == sub + LANES // 2, total[part], 0.0))
                halves.append(jnp.where(sub == 2 * heads, jnp.sum(stat, axis=0, keepdims=True), o[part]))
            return rows, jnp.concatenate(halves, axis=0)

        def compute(wave):
            done = [partials(first // 2 + k) for first, _ in wave for k in range(nx // 2)]
            for rows, part in done:
                send[layer, rows, :] = part

        if layer == 0:
            for wave in waves:
                compute(wave)
            mark('barrier')
            pl.semaphore_wait(barrier, n_sp)
        for wave in waves:
            if layer > 0:
                compute(wave)
            for dst in dests(wave):
                pltpu.make_async_remote_copy(
                    src_ref=send.at[layer, pl.ds(pl.multiple_of(dst * 16, 16), message), :], dst_ref=recv.at[layer, home, :],
                    send_sem=rs_ss.at[layer], recv_sem=rs_rs.at[layer], device_id=at_sp(dst), device_id_type=MESH).start()
        recv[layer, home, :] = send[layer, home, :]
        peers = pl.ds(0, (n_sp - 1) * message)
        rs_all = pltpu.make_async_remote_copy(
            src_ref=send.at[layer, peers, :], dst_ref=recv.at[layer, peers, :],
            send_sem=rs_ss.at[layer], recv_sem=rs_rs.at[layer], device_id=at_sp(me), device_id_type=MESH)
        mark('rswait')
        rs_all.wait_recv()

        mark('merge')
        stats = jnp.transpose(recv[layer, pl.ds(2 * heads, n_sp, stride=16), :])
        tops, totals = stats[0:16], stats[LANES // 2:LANES // 2 + 16]
        weight = jnp.exp(tops - jnp.max(tops, axis=-1, keepdims=True))
        denom = jnp.sum(weight * totals, axis=-1, keepdims=True)
        numer = [jnp.zeros((16, LANES), F32) for _ in range(4)]
        for src in range(n_sp):
            numer[src % 4] = numer[src % 4] + weight[:, src:src + 1] * recv[layer, src * 16:src * 16 + 16, :]
        merged = ((numer[0] + numer[1]) + (numer[2] + numer[3])) / denom
        for t in range(2):
            for h in range(heads):
                pad_a[t:t + 1, h * LANES:(h + 1) * LANES] = merged[t * heads + h:t * heads + h + 1, :]

        mark('wout')
        wo_copy(layer).wait()
        part = dot(pad_a[...].astype(BF16), wo_v[...])[0:8]
        if layer + 1 < n_layers:
            wo_copy(layer + 1).start()
        u1 = (res[0:8, :] + exchange(layer, 0, part)).astype(BF16).astype(F32)
        mark('gateup')
        h2 = rms_norm(jnp.concatenate([u1, jnp.zeros_like(u1)], axis=0), gm[layer:layer + 1, :])

        def gate_up(c, size):
            cols_copy(wg, wg_v, g_sem, layer, c, size).wait()
            cols_copy(wu, wu_v, u_sem, layer, c, size).wait()
            cols = pl.ds(pl.multiple_of(c * chunk, LANES), size)
            gate = dot(h2, wg_v[:, cols])
            up = dot(h2, wu_v[:, cols])
            g_v[:, cols] = (jax.nn.silu(gate) * up).astype(BF16)
            if layer + 1 < n_layers:
                cols_copy(wg, wg_v, g_sem, layer + 1, c, size).start()
                cols_copy(wu, wu_v, u_sem, layer + 1, c, size).start()

        def down(c, size):
            rows_copy(layer, c, size).wait()
            rows = pl.ds(pl.multiple_of(c * chunk, LANES), size)
            acc[...] += dot(g_v[:, rows], wd_v[rows, :])
            if layer + 1 < n_layers:
                rows_copy(layer + 1, c, size).start()

        def loop_of(piece):
            def step(c, carry):
                piece(c, chunk)
                return carry

            lax.fori_loop(0, n_full, step, 0)
            if tail:
                piece(n_full, tail)

        loop_of(gate_up)
        mark('down')
        acc[...] = jnp.zeros_like(acc)
        loop_of(down)
        mark('tp2')
        u2 = (u1 + exchange(layer, 1, acc[0:8, :])).astype(BF16).astype(F32)
        res[0:8, :] = u2

        mark('agsend')
        row = jnp.where(core == 0, u2[0:1], u2[1:2])
        for j in range(blocks):
            ag[layer, j:j + 1, :] = row[:, j * LANES:(j + 1) * LANES]
        home = pl.ds(pl.multiple_of(me * 16, 16), blocks)
        ubuf[layer, core, home, :] = jnp.concatenate([row[:, j * LANES:(j + 1) * LANES] for j in range(blocks)], axis=0)
        for k, wave in enumerate(waves):
            for dst in dests(wave):
                pltpu.make_async_remote_copy(
                    src_ref=ag.at[layer], dst_ref=ubuf.at[layer, core, home, :],
                    send_sem=ag_ss.at[layer], recv_sem=ag_rs.at[layer, k],
                    device_id=at_sp(dst), device_id_type=MESH).start()
        mark('agwait')
        swaps = []
        for k, wave in enumerate(back_waves):
            count = sum(nx - (1 if own else 0) for _, own in wave)
            got = pl.ds(0, count * blocks)
            pltpu.make_async_remote_copy(
                src_ref=ubuf.at[layer, core, got, :], dst_ref=ubuf.at[layer, core, got, :],
                send_sem=ag_ss.at[layer], recv_sem=ag_rs.at[layer, k], device_id=at_sp(me), device_id_type=MESH).wait_recv()
            for q, (first, _) in enumerate(wave):
                rows = pl.ds(pl.multiple_of(first * 16, 16), nx * 16)
                swap = pltpu.make_async_remote_copy(
                    src_ref=ubuf.at[layer, core, rows, :], dst_ref=ubuf.at[layer, core, rows, :],
                    send_sem=dd_ss.at[layer, k, q], recv_sem=dd_rs.at[layer, k, q], device_id={'tp': other}, device_id_type=MESH)
                swap.start()
                swaps.append(swap)
        mark('swap')
        for swap in swaps:
            swap.wait()
        mark('fin')
        got = pl.ds(0, (n_sp - 1) * blocks)
        ag_all = pltpu.make_async_remote_copy(
            src_ref=ubuf.at[layer, core, got, :], dst_ref=ubuf.at[layer, core, got, :],
            send_sem=ag_ss.at[layer], recv_sem=ag_rs.at[layer, 0], device_id=at_sp(me), device_id_type=MESH)
        rs_all.wait_send()
        for copy in stored:
            copy.wait()
        ag_all.wait_send()
        if layer + 1 < n_layers:
            for c in range(2):
                for j in range(blocks):
                    u3[j, pl.ds(c, n_sp, stride=2), :] = ubuf[layer, c, pl.ds(j, n_sp, stride=16), :]
        else:
            for s in range(n_steps):
                for j in range(blocks):
                    rows = pl.ds((s // 2) * 16 + j, n_seq, stride=32)
                    out[s, :, j * LANES:(j + 1) * LANES] = ubuf[layer, s % 2, rows, :].astype(BF16)

    hid = pltpu.make_async_copy(out, bundle.at[pl.ds(0, n_steps)], out_sem.at[2 * n_layers])
    hid.start()
    hid.wait()
    mark(None)


def store_kernel(n_sp, n_steps, len_ref, bundle, kc, vc, hid_out, kc_out, vc_out,
                 hid_v, kv_new, k_tile, v_tile, sems, tile_sems):
    n_layers, n_seq = kc.shape[0], kc.shape[1]
    me = lax.axis_index('sp')
    new_hbm = bundle.at[pl.ds(n_steps, 2 * n_layers), :, pl.ds(0, LANES)]
    pairs = ((new_hbm, kv_new), (bundle.at[pl.ds(0, n_steps)], hid_v), (kc, kc_out), (vc, vc_out))
    copies = [pltpu.make_async_copy(src, dst, sems.at[i]) for i, (src, dst) in enumerate(pairs)]
    for copy in copies:
        copy.start()
    copies[0].wait()
    patches = []
    for layer in range(n_layers):
        k_new, v_new = kv_new[2 * layer].astype(F32), kv_new[2 * layer + 1].astype(F32)
        for b in range(n_seq):
            length = len_ref[b]
            step = lax.rem(me - lax.rem(length, n_sp) + n_sp, n_sp)
            slot = jnp.where(step < n_steps, lax.div(length + step, n_sp), 0)
            tile = pl.ds(pl.multiple_of(lax.div(slot, 16) * 16, 16), 16)
            here = lax.broadcasted_iota(jnp.int32, (16, LANES), 0) == jnp.where(step < n_steps, lax.rem(slot, 16), -1)
            for i, (old, new, buf, dst) in enumerate(((kc, k_new, k_tile, kc_out), (vc, v_new, v_tile, vc_out))):
                buf[layer, b] = jnp.where(here, new[b:b + 1, :], old[layer, b, tile, :].astype(F32)).astype(BF16)
                patches.append(pltpu.make_async_copy(buf.at[layer, b], dst.at[layer, b, tile, :], tile_sems.at[i]))
    copies[1].wait()
    hid_back = pltpu.make_async_copy(hid_v, hid_out, sems.at[4])
    hid_back.start()
    copies[2].wait()
    copies[3].wait()
    for copy in patches:
        copy.start()
    hid_back.wait()
    for copy in patches:
        copy.wait()


def solution(mesh):
    sp_size = mesh.shape['sp']
    dims = (4, 4, 4) if sp_size == 64 else (2, 2, 2)

    def local_fn(tok_emb, lengths, key_cache, val_cache, gain_attn, gain_mlp, w_query, w_key, w_value, w_out, w_gate, w_up, w_down):
        n_steps, n_seq, d_model = tok_emb.shape
        n_layers, _, loc_len, _, head_dim = key_cache.shape
        heads = w_query.shape[2] // head_dim
        ff = w_gate.shape[2]
        n_tok = n_steps * n_seq
        half = np.arange(LANES) % (LANES // 2)
        freq = jnp.asarray((1.0 / ROPE_BASE ** (half * 2.0 / head_dim)).astype(np.float32)[None, :])
        kc = key_cache.reshape(n_layers, n_seq, loc_len, head_dim)
        vc = val_cache.reshape(n_layers, n_seq, loc_len, head_dim)
        cfg = (dims, n_steps, n_layers, n_seq, heads, d_model, ff)
        blocks = d_model // LANES
        n_piece = -(-ff // min(MLP_CHUNK, ff))
        vm, hbm = pl.BlockSpec(memory_space=pltpu.VMEM), pl.BlockSpec(memory_space=pl.ANY)
        dma = pltpu.SemaphoreType.DMA
        bundle = pl.pallas_call(
            functools.partial(decode_kernel, cfg),
            out_shape=jax.ShapeDtypeStruct((160 * n_steps, n_seq, d_model), BF16),
            in_specs=[hbm] * 10 + [vm] * 4,
            out_specs=hbm,
            scratch_shapes=[
                pltpu.VMEM((n_steps, n_seq, d_model), BF16),
                pltpu.VMEM((n_layers, 2, n_seq, LANES), BF16),
                pltpu.VMEM((n_steps, n_seq, d_model), BF16),
                pltpu.VMEM((n_layers, n_seq, loc_len, head_dim), BF16),
                pltpu.VMEM((n_layers, n_seq, loc_len, head_dim), BF16),
                pltpu.VMEM((d_model, (heads + 2) * LANES), BF16),
                pltpu.VMEM((heads * LANES, d_model), BF16),
                pltpu.VMEM((d_model, ff), BF16),
                pltpu.VMEM((d_model, ff), BF16),
                pltpu.VMEM((ff, d_model), BF16),
                pltpu.VMEM((blocks, n_tok, LANES), F32),
                pltpu.VMEM((n_tok * 8, LANES), F32),
                pltpu.VMEM((n_tok * 8, LANES), F32),
                pltpu.VMEM((n_tok * 8, LANES), F32),
                pltpu.VMEM((n_tok, LANES), F32),
                pltpu.VMEM((n_tok, LANES), F32),
                pltpu.VMEM((n_seq, LANES), F32),
                pltpu.VMEM((n_seq, LANES), F32),
                pltpu.VMEM((n_tok, LANES), F32),
                pltpu.VMEM((n_tok, LANES), F32),
                pltpu.VMEM((n_seq, LANES), F32),
                pltpu.VMEM((n_seq, LANES), F32),
                pltpu.VMEM((n_layers, n_tok * 8, LANES), F32),
                pltpu.VMEM((n_layers, n_tok * 8, LANES), F32),
                pltpu.VMEM((16, heads * LANES), F32),
                pltpu.VMEM((16, d_model), F32),
                pltpu.VMEM((16, ff), BF16),
                pltpu.VMEM((16, d_model), F32),
                pltpu.VMEM((n_layers, 2, 8, d_model), F32),
                pltpu.VMEM((n_layers, 2, 8, d_model), F32),
                pltpu.VMEM((n_layers, blocks, LANES), F32),
                pltpu.VMEM((n_layers, 2, sp_size * 16, LANES), F32),
                dma((2 * n_layers + 1,)), dma, dma((n_layers, 2)), dma((3,)), dma, dma((n_piece,)), dma((n_piece,)), dma((n_piece,)),
                dma((n_layers,)), dma((n_layers,)), dma((n_layers, 2)), dma((n_layers, 2)),
                dma((n_layers,)), dma((n_layers, dims[1])), dma((n_layers, dims[1], dims[0])), dma((n_layers, dims[1], dims[0])),
            ],
            compiler_params=pltpu.CompilerParams(collective_id=0, has_side_effects=True, vmem_limit_bytes=VMEM_LIMIT),
            cost_estimate=pl.CostEstimate(flops=24 * 10**9, bytes_accessed=10**8, transcendentals=0),
        )(tok_emb, kc, vc, w_query, w_key, w_value, w_out, w_gate, w_up, w_down, lengths.reshape(1, n_seq), freq, gain_attn, gain_mlp)
        smem = pl.BlockSpec(memory_space=pltpu.SMEM)
        hidden, new_keys, new_vals = pl.pallas_call(
            functools.partial(store_kernel, sp_size, n_steps),
            out_shape=(
                jax.ShapeDtypeStruct((n_steps, n_seq, d_model), BF16),
                jax.ShapeDtypeStruct((n_layers, n_seq, loc_len, head_dim), BF16),
                jax.ShapeDtypeStruct((n_layers, n_seq, loc_len, head_dim), BF16),
            ),
            in_specs=[smem, hbm, vm, vm],
            out_specs=(hbm, hbm, hbm),
            scratch_shapes=[
                pltpu.VMEM((n_steps, n_seq, d_model), BF16),
                pltpu.VMEM((2 * n_layers, n_seq, LANES), BF16),
                pltpu.VMEM((n_layers, n_seq, 16, LANES), BF16),
                pltpu.VMEM((n_layers, n_seq, 16, LANES), BF16),
                dma((5,)), dma((2,)),
            ],
            compiler_params=pltpu.CompilerParams(vmem_limit_bytes=8 * 1024 * 1024),
        )(lengths, bundle, kc, vc)
        return hidden, new_keys.reshape(key_cache.shape), new_vals.reshape(val_cache.shape)

    cache_spec = P(None, 'dp', 'sp', 'tp', None)
    col_spec = P(None, None, 'tp')
    row_spec = P(None, 'tp', None)
    emb_spec = P(None, 'dp', None)
    return jax.shard_map(local_fn, mesh=mesh, in_specs=(emb_spec, P('dp'), cache_spec, cache_spec, P(), P(), col_spec, col_spec, col_spec, row_spec, col_spec, col_spec, row_spec), out_specs=(emb_spec, cache_spec, cache_spec), check_vma=False)
```

```python
import functools
import jax
import jax.numpy as jnp
import numpy as np
from jax import lax
from jax.experimental import pallas as pl
from jax.experimental.pallas import tpu as pltpu
from jax.sharding import PartitionSpec as P

EPS = 1e-5
ROPE_BASE = 500000.0
F32 = jnp.float32
BF16 = jnp.bfloat16
MESH = pl.DeviceIdType.MESH
LANES = 128
VMEM_LIMIT = 59 * 1024 * 1024
MLP_CHUNK = 1280


def rms_norm(x, gain):
    inv_rms = lax.rsqrt(jnp.mean(x * x, axis=-1, keepdims=True) + EPS)
    return (x * inv_rms * gain.astype(F32)).astype(BF16)


def dot(a, b):
    return jnp.dot(a, b, preferred_element_type=F32)


def sin_cos(angle):
    turns = jnp.floor(angle * 0.6366197723675814 + 0.5)
    x = ((angle - turns * 1.5703125) - turns * 4.837512969970703125e-4) - turns * 7.54978995489188216e-8
    z = x * x
    sin_x = x + x * z * ((-1.9515295891e-4 * z + 8.3321608736e-3) * z - 1.6666654611e-1)
    cos_x = 1.0 - 0.5 * z + z * z * ((2.443315711809948e-5 * z - 1.388731625493765e-3) * z + 4.166664568298827e-2)
    quarter = turns - 4.0 * jnp.floor(turns * 0.25)
    odd = (quarter == 1.0) | (quarter == 3.0)
    sin_a = jnp.where(odd, cos_x, sin_x)
    cos_a = jnp.where(odd, sin_x, cos_x)
    sin_a = jnp.where(quarter >= 2.0, -sin_a, sin_a)
    cos_a = jnp.where((quarter == 1.0) | (quarter == 2.0), -cos_a, cos_a)
    return sin_a, cos_a


def decode_kernel(cfg, emb, kc, vc, wq, wk, wv, wo, wg, wu, wd, len_ref, freq_ref, ga, gm,
                  bundle,
                  out, kv_new, emb_v, k_v, v_v, wqkv_v, wo_v, wg_v, wu_v, wd_v, u3, qs, limr, sc, ktok, vtok, ksel, vsel, cos_ref, sin_ref, step_sel, slot_ref,
                  send, recv, pad_a, res, g_v, xs, xr, ag, ubuf,
                  out_sem, in_sem, kv_sem, qkv_sem, wo_sem, g_sem, u_sem, d_sem,
                  rs_ss, rs_rs, x_ss, x_rs, ag_ss, ag_rs, dd_ss, dd_rs):
    dims, n_steps, n_layers, n_seq, heads, d_model, ff = cfg
    nz, ny, nx = dims
    n_sp = nz * ny * nx
    n_tok = n_steps * n_seq
    blocks = d_model // LANES
    q_cols = heads * LANES
    chunk = min(MLP_CHUNK, ff)
    n_full, tail = ff // chunk, ff % chunk
    me = lax.axis_index('sp')
    core = lax.axis_index('tp')
    other = 1 - core

    message = 2 * heads + 1
    my_z, my_y, my_x = me // (ny * nx), lax.rem(me // nx, ny), lax.rem(me, nx)

    def far_first(n):
        return sorted(range(n), key=lambda d: -min(d, n - d))

    def waves_of(sign):
        offsets = [(dz, dy) for dz in far_first(nz) for dy in far_first(ny)]
        offsets = sorted(offsets, key=lambda o: -min(o[0], nz - o[0]) - min(o[1], ny - o[1]))
        rows = []
        for dz, dy in offsets:
            row = lax.rem(my_z + sign * dz + nz, nz) * ny + lax.rem(my_y + sign * dy + ny, ny)
            rows.append((row * nx, dz == 0 and dy == 0))
        return [rows[i:i + nz] for i in range(0, len(rows), nz)]

    waves, back_waves = waves_of(1), waves_of(-1)

    def dests(wave):
        return [first + lax.rem(my_x + dx, nx) for dx in far_first(nx) for first, own in wave if not (own and dx == 0)]

    def at_sp(dst):
        return {'sp': dst}

    scopes = []

    def mark(name):
        if scopes:
            scopes.pop().__exit__(None, None, None)
        if name:
            scope = jax.named_scope(name)
            scope.__enter__()
            scopes.append(scope)

    mark('start')
    def qkv_copies(layer):
        return [
            pltpu.make_async_copy(wq.at[layer], wqkv_v.at[:, pl.ds(0, q_cols)], qkv_sem.at[0]),
            pltpu.make_async_copy(wk.at[layer], wqkv_v.at[:, pl.ds(q_cols, LANES)], qkv_sem.at[1]),
            pltpu.make_async_copy(wv.at[layer], wqkv_v.at[:, pl.ds(q_cols + LANES, LANES)], qkv_sem.at[2]),
        ]

    def kv_copies(layer):
        return [
            pltpu.make_async_copy(kc.at[layer], k_v.at[layer], kv_sem.at[layer, 0]),
            pltpu.make_async_copy(vc.at[layer], v_v.at[layer], kv_sem.at[layer, 1]),
        ]

    def wo_copy(layer):
        return pltpu.make_async_copy(wo.at[layer], wo_v, wo_sem)

    def cols_copy(hbm, vmem, sem, layer, c, size):
        cols = pl.ds(pl.multiple_of(c * chunk, LANES), size)
        return pltpu.make_async_copy(hbm.at[layer, :, cols], vmem.at[:, cols], sem.at[c])

    def rows_copy(layer, c, size):
        rows = pl.ds(pl.multiple_of(c * chunk, LANES), size)
        return pltpu.make_async_copy(wd.at[layer, rows, :], wd_v.at[rows, :], d_sem.at[c])

    pieces = [(c, chunk) for c in range(n_full)] + ([(n_full, tail)] if tail else [])

    emb_copy = pltpu.make_async_copy(emb, emb_v, in_sem)
    emb_copy.start()
    for copy in qkv_copies(0) + kv_copies(0):
        copy.start()
    barrier = pltpu.get_barrier_semaphore()

    for wave in waves:
        for dst in dests(wave):
            pl.semaphore_signal(barrier, inc=1, device_id=at_sp(dst), device_id_type=MESH)
    pl.semaphore_signal(barrier, inc=1, device_id={'tp': other}, device_id_type=MESH)

    eye = lax.broadcasted_iota(jnp.int32, (n_seq, n_seq), 0) == lax.broadcasted_iota(jnp.int32, (n_seq, n_seq), 1)
    lens = jnp.sum(jnp.where(eye, len_ref[...].astype(F32), 0.0), axis=-1, keepdims=True)
    lens = jnp.broadcast_to(lens, (n_seq, LANES))
    me_f = me.astype(F32)
    sel = jnp.full((n_seq, LANES), -1.0, F32)
    for s in range(n_steps):
        pos = lens + float(s)
        row = jnp.floor(pos * (1.0 / n_sp))
        col = pos - row * n_sp
        sel = jnp.where(col == me_f, float(s), sel)
        if s == 0:
            cached = jnp.where(col <= me_f, row - 1.0, row)
            slot_ref[...] = cached + 1.0
        lim = jnp.where(sel >= 0.0, cached + 1.0, cached)
        for h in range(heads):
            limr[pl.ds(s // 2 * 16 + s % 2 * heads + h, n_seq, stride=32), :] = lim
        sin_a, cos_a = sin_cos(pos * freq_ref[...])
        first = lax.broadcasted_iota(jnp.int32, (n_seq, LANES), 1) < LANES // 2
        sin_ref[pl.ds(s, n_seq, stride=n_steps), :] = jnp.where(first, -sin_a, sin_a)
        cos_ref[pl.ds(s, n_seq, stride=n_steps), :] = cos_a
    slot_ref[...] = jnp.where(sel >= 0.0, slot_ref[...], -1.0)
    step_sel[...] = sel
    zeros = jnp.zeros((n_sp, LANES), F32)
    for r in range(2 * heads, 16):
        qs[pl.ds(r, n_sp, stride=16), :] = zeros
        limr[pl.ds(r, n_sp, stride=16), :] = zeros
    pad_a[...] = jnp.zeros_like(pad_a)
    res[...] = jnp.zeros_like(res)

    emb_copy.wait()
    for s in range(n_steps):
        for j in range(blocks):
            u3[j, pl.ds(s, n_seq, stride=n_steps), :] = emb_v[s, :, j * LANES:(j + 1) * LANES].astype(F32)
    for t in range(2):
        for j in range(blocks):
            res[t:t + 1, j * LANES:(j + 1) * LANES] = u3[j, pl.ds(2 * me + t, 1), :]

    def exchange(layer, phase, part):
        xs[layer, phase] = part
        copy = pltpu.make_async_remote_copy(
            src_ref=xs.at[layer, phase], dst_ref=xr.at[layer, phase], send_sem=x_ss.at[layer, phase], recv_sem=x_rs.at[layer, phase],
            device_id={'tp': other}, device_id_type=MESH)
        copy.start()
        copy.wait()
        return part + xr[layer, phase]

    for layer in range(n_layers):
        mark('qkv')
        x = jnp.concatenate([u3[j] for j in range(blocks)], axis=-1)
        normed = rms_norm(x, ga[layer:layer + 1, :])
        for copy in qkv_copies(layer):
            copy.wait()
        if layer == 0:
            wo_copy(0).start()
            for c, size in pieces:
                cols_copy(wg, wg_v, g_sem, 0, c, size).start()
                cols_copy(wu, wu_v, u_sem, 0, c, size).start()
        qkv = dot(normed, wqkv_v[...])
        if layer + 1 < n_layers:
            for copy in qkv_copies(layer + 1):
                copy.start()
        cos_a, sin_a = cos_ref[...], sin_ref[...]

        def rotate(vec):
            return (vec * cos_a + pltpu.roll(vec, LANES // 2, 1) * sin_a).astype(BF16).astype(F32)

        for h in range(heads):
            sc[pl.ds(h * n_tok, n_tok), :] = rotate(qkv[:, h * LANES:(h + 1) * LANES])
        for h in range(heads):
            for t in range(2):
                qs[pl.ds(t * heads + h, n_sp, stride=16), :] = sc[pl.ds(h * n_tok + t, n_sp, stride=2), :]
        ktok[...] = rotate(qkv[:, q_cols:q_cols + LANES])
        vtok[...] = qkv[:, q_cols + LANES:q_cols + 2 * LANES].astype(BF16).astype(F32)
        k_mine = jnp.zeros((n_seq, LANES), F32)
        v_mine = jnp.zeros((n_seq, LANES), F32)
        for s in range(n_steps):
            mine = step_sel[...] == float(s)
            k_mine = jnp.where(mine, ktok[pl.ds(s, n_seq, stride=n_steps), :], k_mine)
            v_mine = jnp.where(mine, vtok[pl.ds(s, n_seq, stride=n_steps), :], v_mine)
        ksel[...] = k_mine
        vsel[...] = v_mine
        kv_new[layer, 0] = k_mine.astype(BF16)
        kv_new[layer, 1] = v_mine.astype(BF16)
        mark('kvwait')
        for copy in kv_copies(layer):
            copy.wait()

        seq_rows = 8 * n_steps
        slot_ids = lax.broadcasted_iota(jnp.int32, (LANES, LANES), 0).astype(F32).astype(BF16)

        def with_new(cache, new, b):
            here = slot_ids == jnp.broadcast_to(slot_ref[pl.ds(b, 1), :].astype(BF16), (LANES, LANES))
            return jnp.where(here, jnp.broadcast_to(new[pl.ds(b, 1), :].astype(BF16), (LANES, LANES)), cache[layer, b])

        stored = [
            pltpu.make_async_copy(kv_new.at[layer, i], bundle.at[n_steps + 2 * layer + i, :, pl.ds(0, LANES)], out_sem.at[2 * layer + i])
            for i in range(2)
        ]
        for copy in stored:
            copy.start()

        mark('values')
        sub = lax.broadcasted_iota(jnp.int32, (16, LANES), 0)
        lane = lax.broadcasted_iota(jnp.int32, (16, LANES), 1)
        home = pl.ds(pl.multiple_of(me * 16, 16), message)

        def partials(b):
            rows = pl.ds(pl.multiple_of(b * seq_rows, seq_rows), seq_rows)
            scores = lax.dot_general(qs[rows, :].astype(BF16), with_new(k_v, ksel, b), (((1,), (1,)), ((), ())),
                                     preferred_element_type=F32)
            valid = lax.broadcasted_iota(jnp.int32, (seq_rows, LANES), 1).astype(F32) <= limr[rows, :]
            scores = jnp.where(valid, scores * LANES ** -0.5, -1e30)
            top = jnp.max(scores, axis=-1, keepdims=True)
            w = jnp.exp(scores - top)
            total = jnp.sum(w, axis=-1, keepdims=True)
            o = dot(w.astype(BF16), with_new(v_v, vsel, b))
            halves = []
            for half in range(2):
                part = slice(16 * half, 16 * half + 16)
                stat = jnp.where(lane == sub, top[part], jnp.where(lane == sub + LANES // 2, total[part], 0.0))
                halves.append(jnp.where(sub == 2 * heads, jnp.sum(stat, axis=0, keepdims=True), o[part]))
            return rows, jnp.concatenate(halves, axis=0)

        def compute(wave):
            done = [partials(first // 2 + k) for first, _ in wave for k in range(nx // 2)]
            for rows, part in done:
                send[layer, rows, :] = part

        if layer == 0:
            for wave in waves:
                compute(wave)
            for c, size in pieces:
                rows_copy(0, c, size).start()
            for copy in kv_copies(1):
                copy.start()
            mark('barrier')
            pl.semaphore_wait(barrier, n_sp)
        for wave in waves:
            if layer > 0:
                compute(wave)
            for dst in dests(wave):
                pltpu.make_async_remote_copy(
                    src_ref=send.at[layer, pl.ds(pl.multiple_of(dst * 16, 16), message), :], dst_ref=recv.at[layer, home, :],
                    send_sem=rs_ss.at[layer], recv_sem=rs_rs.at[layer], device_id=at_sp(dst), device_id_type=MESH).start()
        recv[layer, home, :] = send[layer, home, :]
        peers = pl.ds(0, (n_sp - 1) * message)
        rs_all = pltpu.make_async_remote_copy(
            src_ref=send.at[layer, peers, :], dst_ref=recv.at[layer, peers, :],
            send_sem=rs_ss.at[layer], recv_sem=rs_rs.at[layer], device_id=at_sp(me), device_id_type=MESH)
        mark('rswait')
        rs_all.wait_recv()

        mark('merge')
        stats = jnp.transpose(recv[layer, pl.ds(2 * heads, n_sp, stride=16), :])
        tops, totals = stats[0:16], stats[LANES // 2:LANES // 2 + 16]
        weight = jnp.exp(tops - jnp.max(tops, axis=-1, keepdims=True))
        denom = jnp.sum(weight * totals, axis=-1, keepdims=True)
        numer = [jnp.zeros((16, LANES), F32) for _ in range(4)]
        for src in range(n_sp):
            numer[src % 4] = numer[src % 4] + weight[:, src:src + 1] * recv[layer, src * 16:src * 16 + 16, :]
        merged = ((numer[0] + numer[1]) + (numer[2] + numer[3])) / denom
        for t in range(2):
            for h in range(heads):
                pad_a[t:t + 1, h * LANES:(h + 1) * LANES] = merged[t * heads + h:t * heads + h + 1, :]

        mark('wout')
        wo_copy(layer).wait()
        part = dot(pad_a[...].astype(BF16), wo_v[...])[0:8]
        if layer + 1 < n_layers:
            wo_copy(layer + 1).start()
        u1 = (res[0:8, :] + exchange(layer, 0, part)).astype(BF16).astype(F32)
        mark('gateup')
        h2 = rms_norm(jnp.concatenate([u1, jnp.zeros_like(u1)], axis=0), gm[layer:layer + 1, :])

        for c, size in pieces:
            cols_copy(wg, wg_v, g_sem, layer, c, size).wait()
            cols_copy(wu, wu_v, u_sem, layer, c, size).wait()
        for c, size in pieces:
            cols = pl.ds(c * chunk, size)
            g_v[:, cols] = (jax.nn.silu(dot(h2, wg_v[:, cols])) * dot(h2, wu_v[:, cols])).astype(BF16)
        if layer + 1 < n_layers:
            for c, size in pieces:
                cols_copy(wg, wg_v, g_sem, layer + 1, c, size).start()
                cols_copy(wu, wu_v, u_sem, layer + 1, c, size).start()
        mark('down')
        for c, size in pieces:
            rows_copy(layer, c, size).wait()
        part = jnp.zeros((16, d_model), F32)
        for c, size in pieces:
            rows = pl.ds(c * chunk, size)
            part += dot(g_v[:, rows], wd_v[rows, :])
        if layer + 1 < n_layers:
            for c, size in pieces:
                rows_copy(layer + 1, c, size).start()
        mark('tp2')
        u2 = (u1 + exchange(layer, 1, part[0:8])).astype(BF16).astype(F32)
        res[0:8, :] = u2

        mark('agsend')
        row = jnp.where(core == 0, u2[0:1], u2[1:2])
        for j in range(blocks):
            ag[layer, j:j + 1, :] = row[:, j * LANES:(j + 1) * LANES]
        home = pl.ds(pl.multiple_of(me * 16, 16), blocks)
        ubuf[layer, core, home, :] = jnp.concatenate([row[:, j * LANES:(j + 1) * LANES] for j in range(blocks)], axis=0)
        for k, wave in enumerate(waves):
            for dst in dests(wave):
                pltpu.make_async_remote_copy(
                    src_ref=ag.at[layer], dst_ref=ubuf.at[layer, core, home, :],
                    send_sem=ag_ss.at[layer], recv_sem=ag_rs.at[layer, k],
                    device_id=at_sp(dst), device_id_type=MESH).start()
        mark('agwait')
        swaps = []
        for k, wave in enumerate(back_waves):
            count = sum(nx - (1 if own else 0) for _, own in wave)
            got = pl.ds(0, count * blocks)
            pltpu.make_async_remote_copy(
                src_ref=ubuf.at[layer, core, got, :], dst_ref=ubuf.at[layer, core, got, :],
                send_sem=ag_ss.at[layer], recv_sem=ag_rs.at[layer, k], device_id=at_sp(me), device_id_type=MESH).wait_recv()
            for q, (first, _) in enumerate(wave):
                rows = pl.ds(pl.multiple_of(first * 16, 16), nx * 16)
                swap = pltpu.make_async_remote_copy(
                    src_ref=ubuf.at[layer, core, rows, :], dst_ref=ubuf.at[layer, core, rows, :],
                    send_sem=dd_ss.at[layer, k, q], recv_sem=dd_rs.at[layer, k, q], device_id={'tp': other}, device_id_type=MESH)
                swap.start()
                swaps.append(swap)
        mark('swap')
        for swap in swaps:
            swap.wait()
        mark('fin')
        got = pl.ds(0, (n_sp - 1) * blocks)
        ag_all = pltpu.make_async_remote_copy(
            src_ref=ubuf.at[layer, core, got, :], dst_ref=ubuf.at[layer, core, got, :],
            send_sem=ag_ss.at[layer], recv_sem=ag_rs.at[layer, 0], device_id=at_sp(me), device_id_type=MESH)
        rs_all.wait_send()
        for copy in stored:
            copy.wait()
        ag_all.wait_send()
        if layer + 1 < n_layers:
            for c in range(2):
                for j in range(blocks):
                    u3[j, pl.ds(c, n_sp, stride=2), :] = ubuf[layer, c, pl.ds(j, n_sp, stride=16), :]
        else:
            for s in range(n_steps):
                for j in range(blocks):
                    rows = pl.ds((s // 2) * 16 + j, n_seq, stride=32)
                    out[s, :, j * LANES:(j + 1) * LANES] = ubuf[layer, s % 2, rows, :].astype(BF16)

    hid = pltpu.make_async_copy(out, bundle.at[pl.ds(0, n_steps)], out_sem.at[2 * n_layers])
    hid.start()
    hid.wait()
    mark(None)


def store_kernel(n_sp, n_steps, len_ref, bundle, kc, vc, hid_out, kc_out, vc_out,
                 hid_v, kv_new, k_tile, v_tile, sems, tile_sems):
    n_layers, n_seq = kc.shape[0], kc.shape[1]
    me = lax.axis_index('sp')
    new_hbm = bundle.at[pl.ds(n_steps, 2 * n_layers), :, pl.ds(0, LANES)]
    hid_in = pltpu.make_async_copy(bundle.at[pl.ds(0, n_steps)], hid_v, sems.at[0])
    hid_back = pltpu.make_async_copy(hid_v, hid_out, sems.at[1])
    new_in = pltpu.make_async_copy(new_hbm, kv_new, sems.at[2])
    new_in.start()
    hid_in.start()
    caches = ((kc, k_tile, kc_out), (vc, v_tile, vc_out))
    parts = [(layer, i) for layer in range(n_layers) for i in range(2)]
    whole = [pltpu.make_async_copy(caches[i][0].at[layer], caches[i][2].at[layer], sems.at[3 + 2 * layer + i]) for layer, i in parts]
    for copy in whole:
        copy.start()
    new_in.wait()
    patches = {part: [] for part in parts}
    for b in range(n_seq):
        length = len_ref[b]
        step = lax.rem(me - lax.rem(length, n_sp) + n_sp, n_sp)
        slot = jnp.where(step < n_steps, lax.div(length + step, n_sp), 0)
        tile = pl.ds(pl.multiple_of(lax.div(slot, 16) * 16, 16), 16)
        here = lax.broadcasted_iota(jnp.int32, (16, LANES), 0) == jnp.where(step < n_steps, lax.rem(slot, 16), -1)
        for layer, i in parts:
            old, buf, dst = caches[i]
            new = kv_new[2 * layer + i].astype(F32)[b:b + 1, :]
            buf[layer, b] = jnp.where(here, new, old[layer, b, tile, :].astype(F32)).astype(BF16)
            patches[layer, i].append(pltpu.make_async_copy(buf.at[layer, b], dst.at[layer, b, tile, :], tile_sems.at[0]))
    hid_in.wait()
    hid_back.start()
    for part, copy in zip(parts, whole):
        copy.wait()
        for patch in patches[part]:
            patch.start()
    hid_back.wait()
    for part in parts:
        for patch in patches[part]:
            patch.wait()


def solution(mesh):
    sp_size = mesh.shape['sp']
    dims = (4, 4, 4) if sp_size == 64 else (2, 2, 2)

    def local_fn(tok_emb, lengths, key_cache, val_cache, gain_attn, gain_mlp, w_query, w_key, w_value, w_out, w_gate, w_up, w_down):
        n_steps, n_seq, d_model = tok_emb.shape
        n_layers, _, loc_len, _, head_dim = key_cache.shape
        heads = w_query.shape[2] // head_dim
        ff = w_gate.shape[2]
        n_tok = n_steps * n_seq
        half = np.arange(LANES) % (LANES // 2)
        freq = jnp.asarray((1.0 / ROPE_BASE ** (half * 2.0 / head_dim)).astype(np.float32)[None, :])
        kc = key_cache.reshape(n_layers, n_seq, loc_len, head_dim)
        vc = val_cache.reshape(n_layers, n_seq, loc_len, head_dim)
        cfg = (dims, n_steps, n_layers, n_seq, heads, d_model, ff)
        blocks = d_model // LANES
        n_piece = -(-ff // min(MLP_CHUNK, ff))
        vm, hbm = pl.BlockSpec(memory_space=pltpu.VMEM), pl.BlockSpec(memory_space=pl.ANY)
        dma = pltpu.SemaphoreType.DMA
        bundle = pl.pallas_call(
            functools.partial(decode_kernel, cfg),
            out_shape=jax.ShapeDtypeStruct((160 * n_steps, n_seq, d_model), BF16),
            in_specs=[hbm] * 10 + [vm] * 4,
            out_specs=hbm,
            scratch_shapes=[
                pltpu.VMEM((n_steps, n_seq, d_model), BF16),
                pltpu.VMEM((n_layers, 2, n_seq, LANES), BF16),
                pltpu.VMEM((n_steps, n_seq, d_model), BF16),
                pltpu.VMEM((n_layers, n_seq, loc_len, head_dim), BF16),
                pltpu.VMEM((n_layers, n_seq, loc_len, head_dim), BF16),
                pltpu.VMEM((d_model, (heads + 2) * LANES), BF16),
                pltpu.VMEM((heads * LANES, d_model), BF16),
                pltpu.VMEM((d_model, ff), BF16),
                pltpu.VMEM((d_model, ff), BF16),
                pltpu.VMEM((ff, d_model), BF16),
                pltpu.VMEM((blocks, n_tok, LANES), F32),
                pltpu.VMEM((n_tok * 8, LANES), F32),
                pltpu.VMEM((n_tok * 8, LANES), F32),
                pltpu.VMEM((n_tok * 8, LANES), F32),
                pltpu.VMEM((n_tok, LANES), F32),
                pltpu.VMEM((n_tok, LANES), F32),
                pltpu.VMEM((n_seq, LANES), F32),
                pltpu.VMEM((n_seq, LANES), F32),
                pltpu.VMEM((n_tok, LANES), F32),
                pltpu.VMEM((n_tok, LANES), F32),
                pltpu.VMEM((n_seq, LANES), F32),
                pltpu.VMEM((n_seq, LANES), F32),
                pltpu.VMEM((n_layers, n_tok * 8, LANES), F32),
                pltpu.VMEM((n_layers, n_tok * 8, LANES), F32),
                pltpu.VMEM((16, heads * LANES), F32),
                pltpu.VMEM((16, d_model), F32),
                pltpu.VMEM((16, ff), BF16),
                pltpu.VMEM((n_layers, 2, 8, d_model), F32),
                pltpu.VMEM((n_layers, 2, 8, d_model), F32),
                pltpu.VMEM((n_layers, blocks, LANES), F32),
                pltpu.VMEM((n_layers, 2, sp_size * 16, LANES), F32),
                dma((2 * n_layers + 1,)), dma, dma((n_layers, 2)), dma((3,)), dma, dma((n_piece,)), dma((n_piece,)), dma((n_piece,)),
                dma((n_layers,)), dma((n_layers,)), dma((n_layers, 2)), dma((n_layers, 2)),
                dma((n_layers,)), dma((n_layers, dims[1])), dma((n_layers, dims[1], dims[0])), dma((n_layers, dims[1], dims[0])),
            ],
            compiler_params=pltpu.CompilerParams(collective_id=0, has_side_effects=True, vmem_limit_bytes=VMEM_LIMIT),
            cost_estimate=pl.CostEstimate(flops=24 * 10**9, bytes_accessed=10**8, transcendentals=0),
        )(tok_emb, kc, vc, w_query, w_key, w_value, w_out, w_gate, w_up, w_down, lengths.reshape(1, n_seq), freq, gain_attn, gain_mlp)
        smem = pl.BlockSpec(memory_space=pltpu.SMEM)
        hidden, new_keys, new_vals = pl.pallas_call(
            functools.partial(store_kernel, sp_size, n_steps),
            out_shape=(
                jax.ShapeDtypeStruct((n_steps, n_seq, d_model), BF16),
                jax.ShapeDtypeStruct((n_layers, n_seq, loc_len, head_dim), BF16),
                jax.ShapeDtypeStruct((n_layers, n_seq, loc_len, head_dim), BF16),
            ),
            in_specs=[smem, hbm, vm, vm],
            out_specs=(hbm, hbm, hbm),
            scratch_shapes=[
                pltpu.VMEM((n_steps, n_seq, d_model), BF16),
                pltpu.VMEM((2 * n_layers, n_seq, LANES), BF16),
                pltpu.VMEM((n_layers, n_seq, 16, LANES), BF16),
                pltpu.VMEM((n_layers, n_seq, 16, LANES), BF16),
                dma((3 + 2 * n_layers,)), dma((1,)),
            ],
            compiler_params=pltpu.CompilerParams(vmem_limit_bytes=8 * 1024 * 1024),
        )(lengths, bundle, kc, vc)
        return hidden, new_keys.reshape(key_cache.shape), new_vals.reshape(val_cache.shape)

    cache_spec = P(None, 'dp', 'sp', 'tp', None)
    col_spec = P(None, None, 'tp')
    row_spec = P(None, 'tp', None)
    emb_spec = P(None, 'dp', None)
    return jax.shard_map(local_fn, mesh=mesh, in_specs=(emb_spec, P('dp'), cache_spec, cache_spec, P(), P(), col_spec, col_spec, col_spec, row_spec, col_spec, col_spec, row_spec), out_specs=(emb_spec, cache_spec, cache_spec), check_vma=False)
```

```python
import functools
import jax
import jax.numpy as jnp
import numpy as np
from jax import lax
from jax.experimental import pallas as pl
from jax.experimental.pallas import tpu as pltpu
from jax.sharding import PartitionSpec as P

EPS = 1e-5
ROPE_BASE = 500000.0
F32 = jnp.float32
BF16 = jnp.bfloat16
MESH = pl.DeviceIdType.MESH
LANES = 128
VMEM_LIMIT = 59 * 1024 * 1024
MLP_CHUNK = 1280


def rms_norm(x, gain):
    inv_rms = lax.rsqrt(jnp.mean(x * x, axis=-1, keepdims=True) + EPS)
    return (x * inv_rms * gain.astype(F32)).astype(BF16)


def dot(a, b):
    return jnp.dot(a, b, preferred_element_type=F32)


def sin_cos(angle):
    turns = jnp.floor(angle * 0.6366197723675814 + 0.5)
    x = ((angle - turns * 1.5703125) - turns * 4.837512969970703125e-4) - turns * 7.54978995489188216e-8
    z = x * x
    sin_x = x + x * z * ((-1.9515295891e-4 * z + 8.3321608736e-3) * z - 1.6666654611e-1)
    cos_x = 1.0 - 0.5 * z + z * z * ((2.443315711809948e-5 * z - 1.388731625493765e-3) * z + 4.166664568298827e-2)
    quarter = turns - 4.0 * jnp.floor(turns * 0.25)
    odd = (quarter == 1.0) | (quarter == 3.0)
    sin_a = jnp.where(odd, cos_x, sin_x)
    cos_a = jnp.where(odd, sin_x, cos_x)
    sin_a = jnp.where(quarter >= 2.0, -sin_a, sin_a)
    cos_a = jnp.where((quarter == 1.0) | (quarter == 2.0), -cos_a, cos_a)
    return sin_a, cos_a


def decode_kernel(cfg, emb, kc, vc, wq, wk, wv, wo, wg, wu, wd, len_ref, freq_ref, ga, gm,
                  bundle,
                  out, kv_new, emb_v, k_v, v_v, wqkv_v, wo_v, wg_v, wu_v, wd_v, u3, qs, limr, sc, ktok, vtok, ksel, vsel, cos_ref, sin_ref, step_sel, slot_ref,
                  send, recv, pad_a, res, g_v, xs, xr, ag, ubuf,
                  out_sem, in_sem, kv_sem, qkv_sem, wo_sem, g_sem, u_sem, d_sem,
                  rs_ss, rs_rs, x_ss, x_rs, ag_ss, ag_rs, dd_ss, dd_rs):
    dims, n_steps, n_layers, n_seq, heads, d_model, ff = cfg
    nz, ny, nx = dims
    n_sp = nz * ny * nx
    n_tok = n_steps * n_seq
    blocks = d_model // LANES
    q_cols = heads * LANES
    chunk = min(MLP_CHUNK, ff)
    n_full, tail = ff // chunk, ff % chunk
    me = lax.axis_index('sp')
    core = lax.axis_index('tp')
    other = 1 - core

    message = 2 * heads + 1
    my_z, my_y, my_x = me // (ny * nx), lax.rem(me // nx, ny), lax.rem(me, nx)

    def far_first(n):
        return sorted(range(n), key=lambda d: -min(d, n - d))

    def waves_of(sign):
        offsets = [(dz, dy) for dz in far_first(nz) for dy in far_first(ny)]
        offsets = sorted(offsets, key=lambda o: -min(o[0], nz - o[0]) - min(o[1], ny - o[1]))
        rows = []
        for dz, dy in offsets:
            row = lax.rem(my_z + sign * dz + nz, nz) * ny + lax.rem(my_y + sign * dy + ny, ny)
            rows.append((row * nx, dz == 0 and dy == 0))
        return [rows[i:i + nz] for i in range(0, len(rows), nz)]

    waves, back_waves = waves_of(1), waves_of(-1)

    def dests(wave):
        return [first + lax.rem(my_x + dx, nx) for dx in far_first(nx) for first, own in wave if not (own and dx == 0)]

    def at_sp(dst):
        return {'sp': dst}

    scopes = []

    def mark(name):
        if scopes:
            scopes.pop().__exit__(None, None, None)
        if name:
            scope = jax.named_scope(name)
            scope.__enter__()
            scopes.append(scope)

    mark('start')
    def qkv_copies(layer):
        return [
            pltpu.make_async_copy(wq.at[layer], wqkv_v.at[:, pl.ds(0, q_cols)], qkv_sem.at[0]),
            pltpu.make_async_copy(wk.at[layer], wqkv_v.at[:, pl.ds(q_cols, LANES)], qkv_sem.at[1]),
            pltpu.make_async_copy(wv.at[layer], wqkv_v.at[:, pl.ds(q_cols + LANES, LANES)], qkv_sem.at[2]),
        ]

    def kv_copies(layer):
        return [
            pltpu.make_async_copy(kc.at[layer], k_v.at[layer], kv_sem.at[layer, 0]),
            pltpu.make_async_copy(vc.at[layer], v_v.at[layer], kv_sem.at[layer, 1]),
        ]

    def wo_copy(layer):
        return pltpu.make_async_copy(wo.at[layer], wo_v, wo_sem)

    def cols_copy(hbm, vmem, sem, layer, c, size):
        cols = pl.ds(pl.multiple_of(c * chunk, LANES), size)
        return pltpu.make_async_copy(hbm.at[layer, :, cols], vmem.at[:, cols], sem.at[c])

    def rows_copy(layer, c, size):
        rows = pl.ds(pl.multiple_of(c * chunk, LANES), size)
        return pltpu.make_async_copy(wd.at[layer, rows, :], wd_v.at[rows, :], d_sem.at[c])

    pieces = [(c, chunk) for c in range(n_full)] + ([(n_full, tail)] if tail else [])

    emb_copy = pltpu.make_async_copy(emb, emb_v, in_sem)
    emb_copy.start()
    for copy in qkv_copies(0) + kv_copies(0):
        copy.start()
    barrier = pltpu.get_barrier_semaphore()

    for wave in waves:
        for dst in dests(wave):
            pl.semaphore_signal(barrier, inc=1, device_id=at_sp(dst), device_id_type=MESH)
    pl.semaphore_signal(barrier, inc=1, device_id={'tp': other}, device_id_type=MESH)

    eye = lax.broadcasted_iota(jnp.int32, (n_seq, n_seq), 0) == lax.broadcasted_iota(jnp.int32, (n_seq, n_seq), 1)
    lens = jnp.sum(jnp.where(eye, len_ref[...].astype(F32), 0.0), axis=-1, keepdims=True)
    lens = jnp.broadcast_to(lens, (n_seq, LANES))
    me_f = me.astype(F32)
    sel = jnp.full((n_seq, LANES), -1.0, F32)
    for s in range(n_steps):
        pos = lens + float(s)
        row = jnp.floor(pos * (1.0 / n_sp))
        col = pos - row * n_sp
        sel = jnp.where(col == me_f, float(s), sel)
        if s == 0:
            cached = jnp.where(col <= me_f, row - 1.0, row)
            slot_ref[...] = cached + 1.0
        lim = jnp.where(sel >= 0.0, cached + 1.0, cached)
        for h in range(heads):
            limr[pl.ds(s // 2 * 16 + s % 2 * heads + h, n_seq, stride=32), :] = lim
        sin_a, cos_a = sin_cos(pos * freq_ref[...])
        first = lax.broadcasted_iota(jnp.int32, (n_seq, LANES), 1) < LANES // 2
        sin_ref[pl.ds(s, n_seq, stride=n_steps), :] = jnp.where(first, -sin_a, sin_a)
        cos_ref[pl.ds(s, n_seq, stride=n_steps), :] = cos_a
    slot_ref[...] = jnp.where(sel >= 0.0, slot_ref[...], -1.0)
    step_sel[...] = sel
    zeros = jnp.zeros((n_sp, LANES), F32)
    for r in range(2 * heads, 16):
        qs[pl.ds(r, n_sp, stride=16), :] = zeros
        limr[pl.ds(r, n_sp, stride=16), :] = zeros
    pad_a[...] = jnp.zeros_like(pad_a)
    res[...] = jnp.zeros_like(res)

    emb_copy.wait()
    for s in range(n_steps):
        for j in range(blocks):
            u3[j, pl.ds(s, n_seq, stride=n_steps), :] = emb_v[s, :, j * LANES:(j + 1) * LANES].astype(F32)
    for t in range(2):
        for j in range(blocks):
            res[t:t + 1, j * LANES:(j + 1) * LANES] = u3[j, pl.ds(2 * me + t, 1), :]

    def exchange(layer, phase, part):
        xs[layer, phase] = part
        copy = pltpu.make_async_remote_copy(
            src_ref=xs.at[layer, phase], dst_ref=xr.at[layer, phase], send_sem=x_ss.at[layer, phase], recv_sem=x_rs.at[layer, phase],
            device_id={'tp': other}, device_id_type=MESH)
        copy.start()
        copy.wait()
        return part + xr[layer, phase]

    for layer in range(n_layers):
        mark('qkv')
        x = jnp.concatenate([u3[j] for j in range(blocks)], axis=-1)
        normed = rms_norm(x, ga[layer:layer + 1, :])
        for copy in qkv_copies(layer):
            copy.wait()
        if layer == 0:
            wo_copy(0).start()
            for c, size in pieces:
                cols_copy(wg, wg_v, g_sem, 0, c, size).start()
                cols_copy(wu, wu_v, u_sem, 0, c, size).start()
        qkv = dot(normed, wqkv_v[...])
        if layer + 1 < n_layers:
            for copy in qkv_copies(layer + 1):
                copy.start()
        cos_a, sin_a = cos_ref[...], sin_ref[...]

        def rotate(vec):
            return (vec * cos_a + pltpu.roll(vec, LANES // 2, 1) * sin_a).astype(BF16).astype(F32)

        for h in range(heads):
            sc[pl.ds(h * n_tok, n_tok), :] = rotate(qkv[:, h * LANES:(h + 1) * LANES])
        for h in range(heads):
            for t in range(2):
                qs[pl.ds(t * heads + h, n_sp, stride=16), :] = sc[pl.ds(h * n_tok + t, n_sp, stride=2), :]
        ktok[...] = rotate(qkv[:, q_cols:q_cols + LANES])
        vtok[...] = qkv[:, q_cols + LANES:q_cols + 2 * LANES].astype(BF16).astype(F32)
        k_mine = jnp.zeros((n_seq, LANES), F32)
        v_mine = jnp.zeros((n_seq, LANES), F32)
        for s in range(n_steps):
            mine = step_sel[...] == float(s)
            k_mine = jnp.where(mine, ktok[pl.ds(s, n_seq, stride=n_steps), :], k_mine)
            v_mine = jnp.where(mine, vtok[pl.ds(s, n_seq, stride=n_steps), :], v_mine)
        ksel[...] = k_mine
        vsel[...] = v_mine
        kv_new[layer, 0] = k_mine.astype(BF16)
        kv_new[layer, 1] = v_mine.astype(BF16)
        mark('kvwait')
        for copy in kv_copies(layer):
            copy.wait()

        seq_rows = 8 * n_steps
        slot_ids = lax.broadcasted_iota(jnp.int32, (LANES, LANES), 0).astype(F32).astype(BF16)

        def with_new(cache, new, b):
            here = slot_ids == jnp.broadcast_to(slot_ref[pl.ds(b, 1), :].astype(BF16), (LANES, LANES))
            return jnp.where(here, jnp.broadcast_to(new[pl.ds(b, 1), :].astype(BF16), (LANES, LANES)), cache[layer, b])

        stored = [
            pltpu.make_async_copy(kv_new.at[layer, i], bundle.at[n_steps + 2 * layer + i, :, pl.ds(0, LANES)], out_sem.at[2 * layer + i])
            for i in range(2)
        ]
        for copy in stored:
            copy.start()

        mark('scores')
        for b in range(n_seq):
            rows = pl.ds(b * seq_rows, seq_rows)
            sc[rows, :] = lax.dot_general(qs[rows, :].astype(BF16), with_new(k_v, ksel, b), (((1,), (1,)), ((), ())),
                                          preferred_element_type=F32)
        mark('values')
        sub = lax.broadcasted_iota(jnp.int32, (16, LANES), 0)
        lane = lax.broadcasted_iota(jnp.int32, (16, LANES), 1)
        home = pl.ds(pl.multiple_of(me * 16, 16), message)

        def partials(b):
            rows = pl.ds(pl.multiple_of(b * seq_rows, seq_rows), seq_rows)
            valid = lax.broadcasted_iota(jnp.int32, (seq_rows, LANES), 1).astype(F32) <= limr[rows, :]
            scores = jnp.where(valid, sc[rows, :] * LANES ** -0.5, -1e30)
            top = jnp.max(scores, axis=-1, keepdims=True)
            w = jnp.exp(scores - top)
            total = jnp.sum(w, axis=-1, keepdims=True)
            o = dot(w.astype(BF16), with_new(v_v, vsel, b))
            halves = []
            for half in range(2):
                part = slice(16 * half, 16 * half + 16)
                stat = jnp.where(lane == sub, top[part], jnp.where(lane == sub + LANES // 2, total[part], 0.0))
                halves.append(jnp.where(sub == 2 * heads, jnp.sum(stat, axis=0, keepdims=True), o[part]))
            return rows, jnp.concatenate(halves, axis=0)

        def compute(wave):
            done = [partials(first // 2 + k) for first, _ in wave for k in range(nx // 2)]
            for rows, part in done:
                send[layer, rows, :] = part

        for wave in waves:
            compute(wave)
        if layer == 0:
            for c, size in pieces:
                rows_copy(0, c, size).start()
            for copy in kv_copies(1):
                copy.start()
            mark('barrier')
            pl.semaphore_wait(barrier, n_sp)
        for wave in waves:
            for dst in dests(wave):
                pltpu.make_async_remote_copy(
                    src_ref=send.at[layer, pl.ds(pl.multiple_of(dst * 16, 16), message), :], dst_ref=recv.at[layer, home, :],
                    send_sem=rs_ss.at[layer], recv_sem=rs_rs.at[layer], device_id=at_sp(dst), device_id_type=MESH).start()
        recv[layer, home, :] = send[layer, home, :]
        peers = pl.ds(0, (n_sp - 1) * message)
        rs_all = pltpu.make_async_remote_copy(
            src_ref=send.at[layer, peers, :], dst_ref=recv.at[layer, peers, :],
            send_sem=rs_ss.at[layer], recv_sem=rs_rs.at[layer], device_id=at_sp(me), device_id_type=MESH)
        mark('rswait')
        rs_all.wait_recv()

        mark('merge')
        stats = jnp.transpose(recv[layer, pl.ds(2 * heads, n_sp, stride=16), :])
        tops, totals = stats[0:16], stats[LANES // 2:LANES // 2 + 16]
        weight = jnp.exp(tops - jnp.max(tops, axis=-1, keepdims=True))
        denom = jnp.sum(weight * totals, axis=-1, keepdims=True)
        numer = [jnp.zeros((16, LANES), F32) for _ in range(4)]
        for src in range(n_sp):
            numer[src % 4] = numer[src % 4] + weight[:, src:src + 1] * recv[layer, src * 16:src * 16 + 16, :]
        merged = ((numer[0] + numer[1]) + (numer[2] + numer[3])) / denom
        for t in range(2):
            for h in range(heads):
                pad_a[t:t + 1, h * LANES:(h + 1) * LANES] = merged[t * heads + h:t * heads + h + 1, :]

        mark('wout')
        wo_copy(layer).wait()
        part = dot(pad_a[...].astype(BF16), wo_v[...])[0:8]
        if layer + 1 < n_layers:
            wo_copy(layer + 1).start()
        u1 = (res[0:8, :] + exchange(layer, 0, part)).astype(BF16).astype(F32)
        mark('gateup')
        h2 = rms_norm(jnp.concatenate([u1, jnp.zeros_like(u1)], axis=0), gm[layer:layer + 1, :])

        for c, size in pieces:
            cols_copy(wg, wg_v, g_sem, layer, c, size).wait()
            cols_copy(wu, wu_v, u_sem, layer, c, size).wait()
        for c, size in pieces:
            cols = pl.ds(c * chunk, size)
            g_v[:, cols] = (jax.nn.silu(dot(h2, wg_v[:, cols])) * dot(h2, wu_v[:, cols])).astype(BF16)
        if layer + 1 < n_layers:
            for c, size in pieces:
                cols_copy(wg, wg_v, g_sem, layer + 1, c, size).start()
                cols_copy(wu, wu_v, u_sem, layer + 1, c, size).start()
        mark('down')
        for c, size in pieces:
            rows_copy(layer, c, size).wait()
        part = jnp.zeros((16, d_model), F32)
        for c, size in pieces:
            rows = pl.ds(c * chunk, size)
            part += dot(g_v[:, rows], wd_v[rows, :])
        if layer + 1 < n_layers:
            for c, size in pieces:
                rows_copy(layer + 1, c, size).start()
        mark('tp2')
        u2 = (u1 + exchange(layer, 1, part[0:8])).astype(BF16).astype(F32)
        res[0:8, :] = u2

        mark('agsend')
        row = jnp.where(core == 0, u2[0:1], u2[1:2])
        for j in range(blocks):
            ag[layer, j:j + 1, :] = row[:, j * LANES:(j + 1) * LANES]
        home = pl.ds(pl.multiple_of(me * 16, 16), blocks)
        ubuf[layer, core, home, :] = jnp.concatenate([row[:, j * LANES:(j + 1) * LANES] for j in range(blocks)], axis=0)
        for k, wave in enumerate(waves):
            for dst in dests(wave):
                pltpu.make_async_remote_copy(
                    src_ref=ag.at[layer], dst_ref=ubuf.at[layer, core, home, :],
                    send_sem=ag_ss.at[layer], recv_sem=ag_rs.at[layer, k],
                    device_id=at_sp(dst), device_id_type=MESH).start()
        mark('agwait')
        swaps = []
        for k, wave in enumerate(back_waves):
            count = sum(nx - (1 if own else 0) for _, own in wave)
            got = pl.ds(0, count * blocks)
            pltpu.make_async_remote_copy(
                src_ref=ubuf.at[layer, core, got, :], dst_ref=ubuf.at[layer, core, got, :],
                send_sem=ag_ss.at[layer], recv_sem=ag_rs.at[layer, k], device_id=at_sp(me), device_id_type=MESH).wait_recv()
            for q, (first, _) in enumerate(wave):
                rows = pl.ds(pl.multiple_of(first * 16, 16), nx * 16)
                swap = pltpu.make_async_remote_copy(
                    src_ref=ubuf.at[layer, core, rows, :], dst_ref=ubuf.at[layer, core, rows, :],
                    send_sem=dd_ss.at[layer, k, q], recv_sem=dd_rs.at[layer, k, q], device_id={'tp': other}, device_id_type=MESH)
                swap.start()
                swaps.append(swap)
        mark('swap')
        for swap in swaps:
            swap.wait()
        mark('fin')
        got = pl.ds(0, (n_sp - 1) * blocks)
        ag_all = pltpu.make_async_remote_copy(
            src_ref=ubuf.at[layer, core, got, :], dst_ref=ubuf.at[layer, core, got, :],
            send_sem=ag_ss.at[layer], recv_sem=ag_rs.at[layer, 0], device_id=at_sp(me), device_id_type=MESH)
        rs_all.wait_send()
        for copy in stored:
            copy.wait()
        ag_all.wait_send()
        if layer + 1 < n_layers:
            for c in range(2):
                for j in range(blocks):
                    u3[j, pl.ds(c, n_sp, stride=2), :] = ubuf[layer, c, pl.ds(j, n_sp, stride=16), :]
        else:
            for s in range(n_steps):
                for j in range(blocks):
                    rows = pl.ds((s // 2) * 16 + j, n_seq, stride=32)
                    out[s, :, j * LANES:(j + 1) * LANES] = ubuf[layer, s % 2, rows, :].astype(BF16)

    hid = pltpu.make_async_copy(out, bundle.at[pl.ds(0, n_steps)], out_sem.at[2 * n_layers])
    hid.start()
    hid.wait()
    mark(None)


def store_kernel(n_sp, n_steps, len_ref, bundle, kc, vc, hid_out, kc_out, vc_out,
                 hid_v, kv_new, k_tile, v_tile, sems, tile_sems):
    n_layers, n_seq = kc.shape[0], kc.shape[1]
    me = lax.axis_index('sp')
    new_hbm = bundle.at[pl.ds(n_steps, 2 * n_layers), :, pl.ds(0, LANES)]
    hid_in = pltpu.make_async_copy(bundle.at[pl.ds(0, n_steps)], hid_v, sems.at[0])
    hid_back = pltpu.make_async_copy(hid_v, hid_out, sems.at[1])
    new_in = pltpu.make_async_copy(new_hbm, kv_new, sems.at[2])
    new_in.start()
    hid_in.start()
    caches = ((kc, k_tile, kc_out), (vc, v_tile, vc_out))
    parts = [(layer, i) for layer in range(n_layers) for i in range(2)]
    whole = [pltpu.make_async_copy(caches[i][0].at[layer], caches[i][2].at[layer], sems.at[3 + 2 * layer + i]) for layer, i in parts]
    for copy in whole:
        copy.start()
    new_in.wait()
    patches = {part: [] for part in parts}
    for b in range(n_seq):
        length = len_ref[b]
        step = lax.rem(me - lax.rem(length, n_sp) + n_sp, n_sp)
        slot = jnp.where(step < n_steps, lax.div(length + step, n_sp), 0)
        tile = pl.ds(pl.multiple_of(lax.div(slot, 16) * 16, 16), 16)
        here = lax.broadcasted_iota(jnp.int32, (16, LANES), 0) == jnp.where(step < n_steps, lax.rem(slot, 16), -1)
        for layer, i in parts:
            old, buf, dst = caches[i]
            new = kv_new[2 * layer + i].astype(F32)[b:b + 1, :]
            buf[layer, b] = jnp.where(here, new, old[layer, b, tile, :].astype(F32)).astype(BF16)
            patches[layer, i].append(pltpu.make_async_copy(buf.at[layer, b], dst.at[layer, b, tile, :], tile_sems.at[0]))
    hid_in.wait()
    hid_back.start()
    for part, copy in zip(parts, whole):
        copy.wait()
        for patch in patches[part]:
            patch.start()
    hid_back.wait()
    for part in parts:
        for patch in patches[part]:
            patch.wait()


def solution(mesh):
    sp_size = mesh.shape['sp']
    dims = (4, 4, 4) if sp_size == 64 else (2, 2, 2)

    def local_fn(tok_emb, lengths, key_cache, val_cache, gain_attn, gain_mlp, w_query, w_key, w_value, w_out, w_gate, w_up, w_down):
        n_steps, n_seq, d_model = tok_emb.shape
        n_layers, _, loc_len, _, head_dim = key_cache.shape
        heads = w_query.shape[2] // head_dim
        ff = w_gate.shape[2]
        n_tok = n_steps * n_seq
        half = np.arange(LANES) % (LANES // 2)
        freq = jnp.asarray((1.0 / ROPE_BASE ** (half * 2.0 / head_dim)).astype(np.float32)[None, :])
        kc = key_cache.reshape(n_layers, n_seq, loc_len, head_dim)
        vc = val_cache.reshape(n_layers, n_seq, loc_len, head_dim)
        cfg = (dims, n_steps, n_layers, n_seq, heads, d_model, ff)
        blocks = d_model // LANES
        n_piece = -(-ff // min(MLP_CHUNK, ff))
        vm, hbm = pl.BlockSpec(memory_space=pltpu.VMEM), pl.BlockSpec(memory_space=pl.ANY)
        dma = pltpu.SemaphoreType.DMA
        bundle = pl.pallas_call(
            functools.partial(decode_kernel, cfg),
            out_shape=jax.ShapeDtypeStruct((160 * n_steps, n_seq, d_model), BF16),
            in_specs=[hbm] * 10 + [vm] * 4,
            out_specs=hbm,
            scratch_shapes=[
                pltpu.VMEM((n_steps, n_seq, d_model), BF16),
                pltpu.VMEM((n_layers, 2, n_seq, LANES), BF16),
                pltpu.VMEM((n_steps, n_seq, d_model), BF16),
                pltpu.VMEM((n_layers, n_seq, loc_len, head_dim), BF16),
                pltpu.VMEM((n_layers, n_seq, loc_len, head_dim), BF16),
                pltpu.VMEM((d_model, (heads + 2) * LANES), BF16),
                pltpu.VMEM((heads * LANES, d_model), BF16),
                pltpu.VMEM((d_model, ff), BF16),
                pltpu.VMEM((d_model, ff), BF16),
                pltpu.VMEM((ff, d_model), BF16),
                pltpu.VMEM((blocks, n_tok, LANES), F32),
                pltpu.VMEM((n_tok * 8, LANES), F32),
                pltpu.VMEM((n_tok * 8, LANES), F32),
                pltpu.VMEM((n_tok * 8, LANES), F32),
                pltpu.VMEM((n_tok, LANES), F32),
                pltpu.VMEM((n_tok, LANES), F32),
                pltpu.VMEM((n_seq, LANES), F32),
                pltpu.VMEM((n_seq, LANES), F32),
                pltpu.VMEM((n_tok, LANES), F32),
                pltpu.VMEM((n_tok, LANES), F32),
                pltpu.VMEM((n_seq, LANES), F32),
                pltpu.VMEM((n_seq, LANES), F32),
                pltpu.VMEM((n_layers, n_tok * 8, LANES), F32),
                pltpu.VMEM((n_layers, n_tok * 8, LANES), F32),
                pltpu.VMEM((16, heads * LANES), F32),
                pltpu.VMEM((16, d_model), F32),
                pltpu.VMEM((16, ff), BF16),
                pltpu.VMEM((n_layers, 2, 8, d_model), F32),
                pltpu.VMEM((n_layers, 2, 8, d_model), F32),
                pltpu.VMEM((n_layers, blocks, LANES), F32),
                pltpu.VMEM((n_layers, 2, sp_size * 16, LANES), F32),
                dma((2 * n_layers + 1,)), dma, dma((n_layers, 2)), dma((3,)), dma, dma((n_piece,)), dma((n_piece,)), dma((n_piece,)),
                dma((n_layers,)), dma((n_layers,)), dma((n_layers, 2)), dma((n_layers, 2)),
                dma((n_layers,)), dma((n_layers, dims[1])), dma((n_layers, dims[1], dims[0])), dma((n_layers, dims[1], dims[0])),
            ],
            compiler_params=pltpu.CompilerParams(collective_id=0, has_side_effects=True, vmem_limit_bytes=VMEM_LIMIT),
            cost_estimate=pl.CostEstimate(flops=24 * 10**9, bytes_accessed=10**8, transcendentals=0),
        )(tok_emb, kc, vc, w_query, w_key, w_value, w_out, w_gate, w_up, w_down, lengths.reshape(1, n_seq), freq, gain_attn, gain_mlp)
        smem = pl.BlockSpec(memory_space=pltpu.SMEM)
        hidden, new_keys, new_vals = pl.pallas_call(
            functools.partial(store_kernel, sp_size, n_steps),
            out_shape=(
                jax.ShapeDtypeStruct((n_steps, n_seq, d_model), BF16),
                jax.ShapeDtypeStruct((n_layers, n_seq, loc_len, head_dim), BF16),
                jax.ShapeDtypeStruct((n_layers, n_seq, loc_len, head_dim), BF16),
            ),
            in_specs=[smem, hbm, vm, vm],
            out_specs=(hbm, hbm, hbm),
            scratch_shapes=[
                pltpu.VMEM((n_steps, n_seq, d_model), BF16),
                pltpu.VMEM((2 * n_layers, n_seq, LANES), BF16),
                pltpu.VMEM((n_layers, n_seq, 16, LANES), BF16),
                pltpu.VMEM((n_layers, n_seq, 16, LANES), BF16),
                dma((3 + 2 * n_layers,)), dma((1,)),
            ],
            compiler_params=pltpu.CompilerParams(vmem_limit_bytes=8 * 1024 * 1024),
        )(lengths, bundle, kc, vc)
        return hidden, new_keys.reshape(key_cache.shape), new_vals.reshape(val_cache.shape)

    cache_spec = P(None, 'dp', 'sp', 'tp', None)
    col_spec = P(None, None, 'tp')
    row_spec = P(None, 'tp', None)
    emb_spec = P(None, 'dp', None)
    return jax.shard_map(local_fn, mesh=mesh, in_specs=(emb_spec, P('dp'), cache_spec, cache_spec, P(), P(), col_spec, col_spec, col_spec, row_spec, col_spec, col_spec, row_spec), out_specs=(emb_spec, cache_spec, cache_spec), check_vma=False)
```
